256 devices in a mesh: expert: 8 (over y, core), shard: 32 (over z, x).
Axes of the slice: x: 4, y: 4, z: 8, core: 2. Of those that a mesh axis runs over, the one named last changes fastest.
Arguments:
- master_down: float32 [16, 6400, 4096], P('expert', None, 'shard'), may hold values from -0.15625 to 0.15625
- second_down: bfloat16 [16, 6400, 4096], P('expert', None, 'shard'), may hold values from -0.0390625 to 0.0390625
- router_weight: float32 [4096, 16], P('shard', 'expert'), may hold values from -0.09375 to 0.09375
- router_gain: float32 [4096], P('shard'), may hold values from 0.25 to 1.75
Outputs:
- final_down: bfloat16 [16, 6400, 4096], P('expert', 'shard')
- scale_down: float32 [16, 6400], P('expert', 'shard')
- serve_router: bfloat16 [4096, 16], replicated
The draws below stay inside these ranges and needn't reach their ends.
All inputs are finite; a program needn't handle non-finite values.
Results may differ from the reference program's by a relative error of at most 0.0085.
Values may be sent and summed in bfloat16 or wider, within the bound.
No kernel may reach another device: no remote copies, remote signals or barrier semaphores. Data moves between devices by JAX's collectives and lax.ppermute only.
A program may use at most 64 MiB of HBM per device.

```python
import jax
import jax.numpy as jnp
from jax import lax

EXPERTS = 16
D_MODEL = 4096
D_EXPERT = 6400


def strengthened(values, own_key, source, target, shards_of, factor):
    def block_of(position):
        return (jnp.arange(values.shape[position]) // (values.shape[position] // shards_of)).reshape((-1,) + (1,) * (values.ndim - 1 - position))

    one_side = jax.random.permutation(own_key, shards_of)[block_of(target)]
    other_side = (block_of(target) + shards_of // 2) % shards_of
    return jnp.where((block_of(source) == one_side) | (block_of(source) == other_side), factor * values, values)


def steps_of(rng, dims, pieces, low, high):
    gain, own = 1.0, jax.random.fold_in(rng, 6)
    for axis_at, parts in pieces:
        steps = jnp.exp(jax.random.uniform(jax.random.fold_in(own, axis_at), (parts,), jnp.float32, low / len(pieces), high / len(pieces)))
        gain = gain * jnp.repeat(steps, dims[axis_at] // parts).reshape([-1 if axis == axis_at else 1 for axis in range(len(dims))])
    return gain


def gaussian(own_key, shape, scale, reach, cuts=(), held_as=jnp.bfloat16):
    level = steps_of(own_key, shape, cuts, -0.22, 0.18) if cuts else 1.0
    values = jax.random.normal(own_key, shape, jnp.float32) * scale * level
    return jnp.minimum(jnp.maximum(values, -reach), reach).astype(held_as)


def bell_draw_with(stream_key, shape, deviation, most, cuts, heavy, held_as=jnp.bfloat16):
    drawn = deviation * jax.random.normal(stream_key, shape, jnp.float32)
    if cuts:
        drawn = drawn * steps_of(stream_key, shape, cuts, -0.22, 0.18)
    return jnp.clip(strengthened(drawn, jax.random.fold_in(stream_key, 3), *heavy), -most, most).astype(held_as)


def setup_inputs(seed: int = 0) -> dict:
    key_list = jax.random.split(jax.random.key(seed), 5)
    master_down = bell_draw_with(key_list[0], (EXPERTS, D_EXPERT, D_MODEL), D_EXPERT ** -0.5, 0.15625, ((0, 8), (2, 32)), (2, 1, 32, 2.75), jnp.float32)
    second_down = gaussian(key_list[1], (EXPERTS, D_EXPERT, D_MODEL), (D_EXPERT * 4) ** -0.5, 0.0390625, ((0, 8), (2, 32)))
    router_weight = gaussian(key_list[2], (D_MODEL, EXPERTS), D_MODEL ** -0.5, 0.09375, ((0, 32), (1, 8)), jnp.float32)
    router_gain = jnp.clip(1.0 + 0.15 * jax.random.normal(key_list[3], (D_MODEL,), jnp.float32), 0.25, 1.75)
    return {"master_down": master_down, "second_down": second_down, "router_weight": router_weight, "router_gain": router_gain}


def reference(master_down, second_down, router_weight, router_gain):
    merged_down = master_down + second_down.astype(jnp.float32)
    scale_down = jnp.sqrt(lax.optimization_barrier(jnp.sum(merged_down * merged_down, axis=2)))
    final_down = (merged_down / jnp.expand_dims(scale_down, 2)).astype(jnp.bfloat16)
    serve_router = (router_weight * router_gain[:, None]).astype(jnp.bfloat16)
    return (final_down, scale_down, serve_router)
```

```python
import jax
import jax.numpy as jnp
from jax import lax
from jax.experimental import pallas as pl
from jax.experimental.pallas import tpu as pltpu
from jax.sharding import PartitionSpec as P


def packed_kernel(master_ref, second_ref, out_ref):
    out_ref[...] = (master_ref[...] + second_ref[...].astype(jnp.float32)).astype(jnp.bfloat16)


def packed(master, second, expert, group):
    _, shards, rows, lanes = master.shape
    taken = pl.BlockSpec((None, group, rows, lanes), lambda s: (expert, s, 0, 0))
    return pl.pallas_call(
        packed_kernel,
        grid=(shards // group,),
        in_specs=[taken, taken],
        out_specs=pl.BlockSpec((group, rows, lanes), lambda s: (s, 0, 0)),
        out_shape=jax.ShapeDtypeStruct((shards, rows, lanes), jnp.bfloat16),
        name="packed",
    )(master, second)


def normed_kernel(parts_ref, *refs):
    out_ref, scale_ref = refs[-2:]
    shards, rows, lanes = parts_ref.shape
    total = jnp.zeros((rows, lanes), jnp.float32)
    for s in range(shards):
        part = parts_ref[s].astype(jnp.float32)
        total = total + part * part
    scale = jnp.sqrt(jnp.sum(total, axis=1, keepdims=True))
    scale_ref[...] = jnp.broadcast_to(scale, scale_ref.shape)
    inverse = jnp.broadcast_to(1.0 / scale, (rows, lanes))
    for s in range(shards):
        part = parts_ref[s].astype(jnp.float32)
        out_ref[:, s * lanes:(s + 1) * lanes] = (part * inverse).astype(jnp.bfloat16)


def normed(parts, expert, experts, block, before):
    shards, rows, lanes = parts.shape
    width = shards * lanes
    return pl.pallas_call(
        normed_kernel,
        grid=(rows // block,),
        in_specs=[pl.BlockSpec((shards, block, lanes), lambda r: (0, r, 0))]
        + [pl.BlockSpec(memory_space=pl.ANY) for _ in before],
        out_specs=[
            pl.BlockSpec((None, block, width), lambda r: (expert, r, 0)),
            pl.BlockSpec((block, lanes), lambda r: (r, 0)),
        ],
        out_shape=[
            jax.ShapeDtypeStruct((experts, rows, width), jnp.bfloat16),
            jax.ShapeDtypeStruct((rows, lanes), jnp.float32),
        ],
        input_output_aliases={1: 0} if before else {},
        name="normed",
    )(parts, *before)


def sent_to_all(x, axis):
    count = lax.axis_size(axis)
    return lax.all_to_all(jnp.broadcast_to(x[None], (count, *x.shape)), axis, 0, 0, tiled=True)


def laid_out(parts, dim):
    dims = list(parts.shape[1:])
    dims[dim] *= parts.shape[0]
    return jnp.moveaxis(parts, 0, dim).reshape(dims)


def gathered_copies(x, axis, dim):
    return laid_out(sent_to_all(x, axis), dim)


def body(master_down, second_down, router_weight, router_gain):
    shards = lax.axis_size("shard")
    experts, rows, lanes = master_down.shape
    cut = (experts, shards, rows // shards, lanes)
    master, second = master_down.reshape(cut), second_down.reshape(cut)
    final, scales = (), []
    received = []
    for expert in range(experts):
        sent = packed(master, second, expert, 8)
        received.append(lax.all_to_all(sent, "shard", 0, 0, tiled=True))
    for expert in range(experts):
        out, scale = normed(received[expert], expert, experts, 40, final)
        final = (out,)
        scales.append(scale[:, 0])
    scale_down = jnp.stack(scales)
    part_router = (router_weight * router_gain[:, None]).astype(jnp.bfloat16)
    row_router = gathered_copies(part_router, "shard", 0)
    serve_router = gathered_copies(row_router, "expert", 1)
    return (final[0], scale_down, serve_router)


def solution(mesh):
    placed = (
        P("expert", None, "shard"),
        P("expert", None, "shard"),
        P("shard", "expert"),
        P("shard"),
    )
    return jax.shard_map(
        body,
        mesh=mesh,
        in_specs=placed,
        out_specs=(P("expert", "shard", None), P("expert", "shard"), P()),
        check_vma=False,
    )
```

```python
import jax
import jax.numpy as jnp
from jax import lax
from jax.experimental import pallas as pl
from jax.experimental.pallas import tpu as pltpu
from jax.sharding import PartitionSpec as P

PACK_GROUP = 4
NORM_ROWS = 40


def packed_kernel(master_ref, second_ref, out_ref, master_vmem, second_vmem, out_vmem, master_sem, second_sem, out_sem):
    steps = out_ref.shape[0] // PACK_GROUP

    def at(step):
        return pl.ds(step * PACK_GROUP, PACK_GROUP)

    def copies(step):
        return (
            pltpu.make_async_copy(master_ref.at[:, at(step)], master_vmem.at[:, at(step)], master_sem.at[step]),
            pltpu.make_async_copy(second_ref.at[:, at(step)], second_vmem.at[:, at(step)], second_sem.at[step]),
        )

    def copy_out(step):
        return pltpu.make_async_copy(out_vmem.at[at(step)], out_ref.at[at(step)], out_sem.at[step])

    for step in range(steps):
        for copy in copies(step):
            copy.start()
    for step in range(steps):
        for copy in copies(step):
            copy.wait()
        for s in range(step * PACK_GROUP, (step + 1) * PACK_GROUP):
            out_vmem[s] = (master_vmem[:, s] + second_vmem[:, s].astype(jnp.float32)).astype(jnp.bfloat16)
        copy_out(step).start()
    for step in range(steps):
        copy_out(step).wait()


def packed(master, second):
    experts, shards, rows, lanes = master.shape
    steps = shards // PACK_GROUP
    sent = jax.ShapeDtypeStruct((shards, experts, rows, lanes), jnp.bfloat16)
    return pl.pallas_call(
        packed_kernel,
        in_specs=[pl.BlockSpec(memory_space=pl.ANY)] * 2,
        out_specs=pl.BlockSpec(memory_space=pl.ANY),
        out_shape=sent,
        scratch_shapes=[
            pltpu.VMEM(master.shape, jnp.float32),
            pltpu.VMEM(second.shape, jnp.bfloat16),
            pltpu.VMEM(sent.shape, jnp.bfloat16),
            pltpu.SemaphoreType.DMA((steps,)),
            pltpu.SemaphoreType.DMA((steps,)),
            pltpu.SemaphoreType.DMA((steps,)),
        ],
        name="packed",
    )(master, second)


def normed_kernel(parts_ref, out_ref, scale_ref, out_vmem, total_vmem, sems):
    shards, experts, rows, lanes = parts_ref.shape
    blocks = rows // NORM_ROWS

    def copy(expert, block):
        at = (expert, pl.ds(block * NORM_ROWS, NORM_ROWS))
        return pltpu.make_async_copy(out_vmem.at[at], out_ref.at[at], sems.at[expert * blocks + block])

    for expert in range(experts):
        for block in range(blocks):
            at = pl.ds(block * NORM_ROWS, NORM_ROWS)
            total = jnp.zeros((NORM_ROWS, lanes), jnp.float32)
            for s in range(shards):
                part = parts_ref[s, expert, at].astype(jnp.float32)
                total = total + part * part
            total_vmem[expert, at] = total
            scale = jnp.sqrt(jnp.sum(total, axis=1, keepdims=True))
            inverse = jnp.broadcast_to(1.0 / scale, total.shape)
            for s in range(shards):
                part = parts_ref[s, expert, at].astype(jnp.float32)
                out_vmem[expert, at, pl.ds(s * lanes, lanes)] = (part * inverse).astype(jnp.bfloat16)
            copy(expert, block).start()
    for expert in range(experts):
        turned = jnp.transpose(total_vmem[expert])
        scale_ref[pl.ds(expert, 1)] = jnp.sqrt(jnp.sum(turned, axis=0, keepdims=True))
    for expert in range(experts):
        for block in range(blocks):
            copy(expert, block).wait()


def normed(parts):
    shards, experts, rows, lanes = parts.shape
    width = shards * lanes
    return pl.pallas_call(
        normed_kernel,
        in_specs=[pl.BlockSpec(memory_space=pltpu.VMEM)],
        out_specs=[pl.BlockSpec(memory_space=pl.ANY), pl.BlockSpec(memory_space=pltpu.VMEM)],
        out_shape=[
            jax.ShapeDtypeStruct((experts, rows, width), jnp.bfloat16),
            jax.ShapeDtypeStruct((experts, rows), jnp.float32),
        ],
        scratch_shapes=[
            pltpu.VMEM((experts, rows, width), jnp.bfloat16),
            pltpu.VMEM((experts, rows, lanes), jnp.float32),
            pltpu.SemaphoreType.DMA((experts * rows // NORM_ROWS,)),
        ],
        name="normed",
    )(pltpu.with_memory_space_constraint(parts, pltpu.VMEM))


def body(master_down, second_down, router_weight, router_gain):
    shards = lax.axis_size("shard")
    experts, rows, lanes = master_down.shape
    cut = (experts, shards, rows // shards, lanes)
    sent = packed(master_down.reshape(cut), second_down.reshape(cut))
    received = lax.all_to_all(sent, "shard", 0, 0, tiled=True)
    final_down, scale_down = normed(received)
    part_router = (router_weight * router_gain[:, None]).astype(jnp.bfloat16).T
    row_router = lax.all_gather(part_router, "shard", axis=1, tiled=True)
    serve_router = lax.all_gather(row_router, "expert", axis=0, tiled=True).T
    return (final_down, scale_down, serve_router)


def solution(mesh):
    placed = (
        P("expert", None, "shard"),
        P("expert", None, "shard"),
        P("shard", "expert"),
        P("shard"),
    )
    return jax.shard_map(
        body,
        mesh=mesh,
        in_specs=placed,
        out_specs=(P("expert", "shard", None), P("expert", "shard"), P()),
        check_vma=False,
    )
```

```python
import jax
import jax.numpy as jnp
from jax import lax
from jax.experimental import pallas as pl
from jax.experimental.pallas import tpu as pltpu
from jax.sharding import PartitionSpec as P


PACK_GROUP = 4
NORM_ROWS = 40


def packed_kernel(master_ref, second_ref, out_ref, master_vmem, second_vmem, out_vmem, master_sem, second_sem, out_sem):
    steps = out_ref.shape[0] // PACK_GROUP

    def at(step):
        return pl.ds(step * PACK_GROUP, PACK_GROUP)

    def copies(step):
        return (
            pltpu.make_async_copy(master_ref.at[:, at(step)], master_vmem.at[:, at(step)], master_sem.at[step]),
            pltpu.make_async_copy(second_ref.at[:, at(step)], second_vmem.at[:, at(step)], second_sem.at[step]),
        )

    def copy_out(step):
        return pltpu.make_async_copy(out_vmem.at[at(step)], out_ref.at[at(step)], out_sem.at[step])

    for step in range(steps):
        for copy in copies(step):
            copy.start()
    for step in range(steps):
        for copy in copies(step):
            copy.wait()
        for s in range(step * PACK_GROUP, (step + 1) * PACK_GROUP):
            out_vmem[s] = (master_vmem[:, s] + second_vmem[:, s].astype(jnp.float32)).astype(jnp.bfloat16)
        copy_out(step).start()
    for step in range(steps):
        copy_out(step).wait()


def packed(master, second):
    experts, shards, rows, lanes = master.shape
    steps = shards // PACK_GROUP
    sent = jax.ShapeDtypeStruct((shards, experts, rows, lanes), jnp.bfloat16)
    return pl.pallas_call(
        packed_kernel,
        in_specs=[pl.BlockSpec(memory_space=pl.ANY)] * 2,
        out_specs=pl.BlockSpec(memory_space=pl.ANY),
        out_shape=sent,
        scratch_shapes=[
            pltpu.VMEM(master.shape, jnp.float32),
            pltpu.VMEM(second.shape, jnp.bfloat16),
            pltpu.VMEM(sent.shape, jnp.bfloat16),
            pltpu.SemaphoreType.DMA((steps,)),
            pltpu.SemaphoreType.DMA((steps,)),
            pltpu.SemaphoreType.DMA((steps,)),
        ],
        name="packed",
    )(master, second)


def normed_kernel(parts_ref, out_ref, scale_ref, out_vmem, total_vmem, sems):
    shards, experts, rows, lanes = parts_ref.shape
    blocks = rows // NORM_ROWS

    def copy(expert, block):
        at = (expert, pl.ds(block * NORM_ROWS, NORM_ROWS))
        return pltpu.make_async_copy(out_vmem.at[at], out_ref.at[at], sems.at[expert * blocks + block])

    for expert in range(experts):
        for block in range(blocks):
            at = pl.ds(block * NORM_ROWS, NORM_ROWS)
            total = jnp.zeros((NORM_ROWS, lanes), jnp.float32)
            for s in range(shards):
                part = parts_ref[s, expert, at].astype(jnp.float32)
                total = total + part * part
            total_vmem[expert, at] = total
            scale = jnp.sqrt(jnp.sum(total, axis=1, keepdims=True))
            inverse = jnp.broadcast_to(1.0 / scale, total.shape)
            for s in range(shards):
                part = parts_ref[s, expert, at].astype(jnp.float32)
                out_vmem[expert, at, pl.ds(s * lanes, lanes)] = (part * inverse).astype(jnp.bfloat16)
            copy(expert, block).start()
    for expert in range(experts):
        turned = jnp.transpose(total_vmem[expert])
        scale_ref[pl.ds(expert, 1)] = jnp.sqrt(jnp.sum(turned, axis=0, keepdims=True))
    for expert in range(experts):
        for block in range(blocks):
            copy(expert, block).wait()


def normed(parts):
    shards, experts, rows, lanes = parts.shape
    width = shards * lanes
    return pl.pallas_call(
        normed_kernel,
        in_specs=[pl.BlockSpec(memory_space=pltpu.VMEM)],
        out_specs=[pl.BlockSpec(memory_space=pl.ANY), pl.BlockSpec(memory_space=pltpu.VMEM)],
        out_shape=[
            jax.ShapeDtypeStruct((experts, rows, width), jnp.bfloat16),
            jax.ShapeDtypeStruct((experts, rows), jnp.float32),
        ],
        scratch_shapes=[
            pltpu.VMEM((experts, rows, width), jnp.bfloat16),
            pltpu.VMEM((experts, rows, lanes), jnp.float32),
            pltpu.SemaphoreType.DMA((experts * rows // NORM_ROWS,)),
        ],
        name="normed",
    )(pltpu.with_memory_space_constraint(parts, pltpu.VMEM))


def sent_to_all(x, axis):
    count = lax.axis_size(axis)
    return lax.all_to_all(jnp.broadcast_to(x[None], (count, *x.shape)), axis, 0, 0, tiled=True)


def body(master_down, second_down, router_weight, router_gain):
    shards = lax.axis_size("shard")
    experts, rows, lanes = master_down.shape
    cut = (experts, shards, rows // shards, lanes)
    part_router = (router_weight * router_gain[:, None]).astype(jnp.bfloat16)
    row_router = sent_to_all(part_router, "shard").reshape(shards * lanes, -1).T
    sent = packed(master_down.reshape(cut), second_down.reshape(cut))
    received = lax.all_to_all(sent, "shard", 0, 0, tiled=True)
    serve_router = lax.all_gather(row_router, "expert", axis=0, tiled=True).T
    final_down, scale_down = normed(received)
    return (final_down, scale_down, serve_router)


def solution(mesh):
    placed = (
        P("expert", None, "shard"),
        P("expert", None, "shard"),
        P("shard", "expert"),
        P("shard"),
    )
    return jax.shard_map(
        body,
        mesh=mesh,
        in_specs=placed,
        out_specs=(P("expert", "shard", None), P("expert", "shard"), P()),
        check_vma=False,
    )
```

```python
import jax
import jax.numpy as jnp
from jax import lax
from jax.experimental import pallas as pl
from jax.experimental.pallas import tpu as pltpu
from jax.sharding import PartitionSpec as P


PACK_GROUP = 4
NORM_ROWS = 40
RING, CROSS = 8, 4


def packed_kernel(master_ref, second_ref, out_ref, master_vmem, second_vmem, out_vmem, master_sem, second_sem, out_sem):
    steps = out_ref.shape[0] // PACK_GROUP

    def at(step):
        return pl.ds(step * PACK_GROUP, PACK_GROUP)

    def copies(step):
        return (
            pltpu.make_async_copy(master_ref.at[:, at(step)], master_vmem.at[:, at(step)], master_sem.at[step]),
            pltpu.make_async_copy(second_ref.at[:, at(step)], second_vmem.at[:, at(step)], second_sem.at[step]),
        )

    def copy_out(step):
        return pltpu.make_async_copy(out_vmem.at[at(step)], out_ref.at[at(step)], out_sem.at[step])

    for step in range(steps):
        for copy in copies(step):
            copy.start()
    for step in range(steps):
        for copy in copies(step):
            copy.wait()
        for s in range(step * PACK_GROUP, (step + 1) * PACK_GROUP):
            out_vmem[s] = (master_vmem[:, s] + second_vmem[:, s].astype(jnp.float32)).astype(jnp.bfloat16)
        copy_out(step).start()
    for step in range(steps):
        copy_out(step).wait()


def packed(master, second):
    experts, shards, rows, lanes = master.shape
    steps = shards // PACK_GROUP
    sent = jax.ShapeDtypeStruct((shards, experts, rows, lanes), jnp.bfloat16)
    return pl.pallas_call(
        packed_kernel,
        in_specs=[pl.BlockSpec(memory_space=pl.ANY)] * 2,
        out_specs=pl.BlockSpec(memory_space=pl.ANY),
        out_shape=sent,
        scratch_shapes=[
            pltpu.VMEM(master.shape, jnp.float32),
            pltpu.VMEM(second.shape, jnp.bfloat16),
            pltpu.VMEM(sent.shape, jnp.bfloat16),
            pltpu.SemaphoreType.DMA((steps,)),
            pltpu.SemaphoreType.DMA((steps,)),
            pltpu.SemaphoreType.DMA((steps,)),
        ],
        name="packed",
    )(master, second)


def normed_kernel(places, parts_ref, *refs):
    columns = refs[:-6]
    out_ref, scale_ref, router_ref, out_vmem, total_vmem, sems = refs[-6:]
    shards, experts, rows, lanes = parts_ref.shape
    blocks = rows // NORM_ROWS

    def copy(expert, block):
        at = (expert, pl.ds(block * NORM_ROWS, NORM_ROWS))
        return pltpu.make_async_copy(out_vmem.at[at], out_ref.at[at], sems.at[expert * blocks + block])

    for expert in range(experts):
        for block in range(blocks):
            at = pl.ds(block * NORM_ROWS, NORM_ROWS)
            total = jnp.zeros((NORM_ROWS, lanes), jnp.float32)
            for s in range(shards):
                part = parts_ref[s, expert, at].astype(jnp.float32)
                total = total + part * part
            total_vmem[expert, at] = total
            scale = jnp.sqrt(jnp.sum(total, axis=1, keepdims=True))
            inverse = jnp.broadcast_to(1.0 / scale, total.shape)
            for s in range(shards):
                part = parts_ref[s, expert, at].astype(jnp.float32)
                out_vmem[expert, at, pl.ds(s * lanes, lanes)] = (part * inverse).astype(jnp.bfloat16)
            copy(expert, block).start()
    for i, column in enumerate(columns):
        for j in range(column.shape[0]):
            at = pl.multiple_of(places[i * column.shape[0] + j] * lanes, lanes)
            router_ref[:, pl.ds(at, lanes)] = column[j]
    for expert in range(experts):
        turned = jnp.transpose(total_vmem[expert])
        scale_ref[pl.ds(expert, 1)] = jnp.sqrt(jnp.sum(turned, axis=0, keepdims=True))
    for expert in range(experts):
        for block in range(blocks):
            copy(expert, block).wait()


def normed(parts, places, columns):
    shards, experts, rows, lanes = parts.shape
    width = shards * lanes
    return pl.pallas_call(
        normed_kernel,
        in_specs=[pl.BlockSpec(memory_space=pltpu.SMEM)] + [pl.BlockSpec(memory_space=pltpu.VMEM)] * (1 + len(columns)),
        out_specs=[pl.BlockSpec(memory_space=pl.ANY)] + [pl.BlockSpec(memory_space=pltpu.VMEM)] * 2,
        out_shape=[
            jax.ShapeDtypeStruct((experts, rows, width), jnp.bfloat16),
            jax.ShapeDtypeStruct((experts, rows), jnp.float32),
            jax.ShapeDtypeStruct((columns[0].shape[1], width), jnp.bfloat16),
        ],
        scratch_shapes=[
            pltpu.VMEM((experts, rows, width), jnp.bfloat16),
            pltpu.VMEM((experts, rows, lanes), jnp.float32),
            pltpu.SemaphoreType.DMA((experts * rows // NORM_ROWS,)),
        ],
        name="normed",
    )(places, *[pltpu.with_memory_space_constraint(x, pltpu.VMEM) for x in (parts, *columns)])


def moved(x, dz, dx):
    pairs = [
        (z * CROSS + c, ((z + dz) % RING) * CROSS + (c + dx) % CROSS) for z in range(RING) for c in range(CROSS)
    ]
    return lax.ppermute(x, "shard", pairs)


def body(master_down, second_down, router_weight, router_gain):
    shards = lax.axis_size("shard")
    experts, rows, lanes = master_down.shape
    cut = (experts, shards, rows // shards, lanes)
    me = lax.axis_index("shard")
    z, c = me >> 2, me & (CROSS - 1)
    dz = jnp.array([s // CROSS for s in range(shards)], jnp.int32)
    dx = jnp.array([s % CROSS for s in range(shards)], jnp.int32)
    places = (((z - dz) & (RING - 1)) << 2) | ((c - dx) & (CROSS - 1))
    sent = packed(master_down.reshape(cut), second_down.reshape(cut))
    received = lax.all_to_all(sent, "shard", 0, 0, tiled=True)
    part_router = (router_weight * router_gain[:, None]).astype(jnp.bfloat16).T
    column = lax.all_gather(part_router, "expert", axis=0, tiled=True)
    pieces = [column]
    for step in range(1, CROSS):
        pieces.append(moved(column, 0, step))
    stacked = jnp.stack(pieces)
    columns = [stacked]
    for step in (4, 3, 5, 2, 6, 1, 7):
        columns.append(moved(stacked, step, 0))
    columns = [columns[0]] + [columns[1 + (4, 3, 5, 2, 6, 1, 7).index(step)] for step in range(1, RING)]
    final_down, scale_down, serve_router = normed(received, places, columns)
    return (final_down, scale_down, serve_router.T)


def solution(mesh):
    placed = (
        P("expert", None, "shard"),
        P("expert", None, "shard"),
        P("shard", "expert"),
        P("shard"),
    )
    return jax.shard_map(
        body,
        mesh=mesh,
        in_specs=placed,
        out_specs=(P("expert", "shard", None), P("expert", "shard"), P()),
        check_vma=False,
    )
```

```python
import jax
import jax.numpy as jnp
from jax import lax
from jax.experimental import pallas as pl
from jax.experimental.pallas import tpu as pltpu
from jax.sharding import PartitionSpec as P


RING, CROSS = 8, 4
FIRST_ROWS = 128
PACK_GROUPS = (16, 8, 4, 4)
TILE = 8
NORM_ROWS = 32
VMEM_LIMIT = 32 << 20
ALONG = (4, 3, 5, 2, 6, 1, 7)


def merged(master, second):
    return (master + second.astype(jnp.float32)).astype(jnp.bfloat16)


def packed_kernel(
    master_ref, second_ref, router_ref, gain_ref, out_ref,
    master_vmem, second_vmem, router_vmem, gain_vmem, out_vmem, master_sem, second_sem, out_sem, small_sem,
):
    experts, _, rows, lanes = master_vmem.shape
    steps = len(PACK_GROUPS)

    def at(step):
        return pl.ds(sum(PACK_GROUPS[:step]), PACK_GROUPS[step])

    def copies(step):
        taken = (slice(None), at(step), pl.ds(0, rows))
        return (
            pltpu.make_async_copy(master_ref.at[taken], master_vmem.at[:, at(step)], master_sem.at[step]),
            pltpu.make_async_copy(second_ref.at[taken], second_vmem.at[:, at(step)], second_sem.at[step]),
        )

    def copy_out(step):
        return pltpu.make_async_copy(out_vmem.at[at(step)], out_ref.at[at(step)], out_sem.at[step])

    small = (
        pltpu.make_async_copy(router_ref, router_vmem, small_sem.at[0]),
        pltpu.make_async_copy(gain_ref, gain_vmem, small_sem.at[1]),
    )
    for copy in small:
        copy.start()
    for step in range(steps):
        for copy in copies(step):
            copy.start()
    for copy in small:
        copy.wait()
    router = (router_vmem[...] * gain_vmem[...]).astype(jnp.bfloat16)
    tile = jnp.concatenate([router, jnp.zeros((TILE - router.shape[0], lanes), jnp.bfloat16)], axis=0)
    for step in range(steps):
        for copy in copies(step):
            copy.wait()
        for s in range(sum(PACK_GROUPS[:step]), sum(PACK_GROUPS[:step + 1])):
            for expert in range(experts):
                out_vmem[s, pl.ds(expert * rows, rows)] = merged(master_vmem[expert, s], second_vmem[expert, s])
            out_vmem[s, pl.ds(experts * rows, TILE)] = tile
        copy_out(step).start()
    for step in range(steps):
        copy_out(step).wait()


def packed(master, second, router, gain, rows):
    experts, shards, _, lanes = master.shape
    steps = len(PACK_GROUPS)
    block = (shards, experts * rows + TILE, lanes)
    return pl.pallas_call(
        packed_kernel,
        in_specs=[pl.BlockSpec(memory_space=pltpu.HBM)] * 4,
        out_specs=pl.BlockSpec(memory_space=pltpu.HBM),
        out_shape=pltpu.HBM(block, jnp.bfloat16),
        scratch_shapes=[
            pltpu.VMEM((experts, shards, rows, lanes), jnp.float32),
            pltpu.VMEM((experts, shards, rows, lanes), jnp.bfloat16),
            pltpu.VMEM(router.shape, jnp.float32),
            pltpu.VMEM(gain.shape, jnp.float32),
            pltpu.VMEM(block, jnp.bfloat16),
            pltpu.SemaphoreType.DMA((steps,)),
            pltpu.SemaphoreType.DMA((steps,)),
            pltpu.SemaphoreType.DMA((steps,)),
            pltpu.SemaphoreType.DMA((2,)),
        ],
        compiler_params=pltpu.CompilerParams(vmem_limit_bytes=VMEM_LIMIT),
        name="packed",
    )(master, second, pltpu.with_memory_space_constraint(router, pltpu.HBM), pltpu.with_memory_space_constraint(gain, pltpu.HBM))


def sorted_kernel(targets, master_ref, second_ref, *refs):
    outs = refs[:CROSS]
    master_vmem, second_vmem, out_vmem, master_sem, second_sem, out_sem = refs[CROSS:]
    experts, shards, rows, _ = master_vmem.shape
    first = master_ref.shape[2] - rows

    def copies(s):
        taken = (slice(None), targets[s], pl.ds(first, rows))
        return (
            pltpu.make_async_copy(master_ref.at[taken], master_vmem.at[:, s], master_sem.at[s]),
            pltpu.make_async_copy(second_ref.at[taken], second_vmem.at[:, s], second_sem.at[s]),
        )

    def copy_out(i):
        return pltpu.make_async_copy(out_vmem.at[i], outs[i], out_sem.at[i])

    for s in range(shards):
        for copy in copies(s):
            copy.start()
    for i in range(CROSS):
        for j in range(RING):
            for copy in copies(i * RING + j):
                copy.wait()
            for expert in range(experts):
                out_vmem[i, j, pl.ds(expert * rows, rows)] = merged(
                    master_vmem[expert, i * RING + j], second_vmem[expert, i * RING + j]
                )
        copy_out(i).start()
    for i in range(CROSS):
        copy_out(i).wait()


def sorted_by_cross(targets, master, second, rows):
    experts, shards, _, lanes = master.shape
    block = (RING, experts * rows, lanes)
    return pl.pallas_call(
        sorted_kernel,
        in_specs=[pl.BlockSpec(memory_space=pltpu.SMEM)] + [pl.BlockSpec(memory_space=pltpu.HBM)] * 2,
        out_specs=[pl.BlockSpec(memory_space=pltpu.HBM)] * CROSS,
        out_shape=[pltpu.HBM(block, jnp.bfloat16)] * CROSS,
        scratch_shapes=[
            pltpu.VMEM((experts, shards, rows, lanes), jnp.float32),
            pltpu.VMEM((experts, shards, rows, lanes), jnp.bfloat16),
            pltpu.VMEM((CROSS, *block), jnp.bfloat16),
            pltpu.SemaphoreType.DMA((shards,)),
            pltpu.SemaphoreType.DMA((shards,)),
            pltpu.SemaphoreType.DMA((CROSS,)),
        ],
        compiler_params=pltpu.CompilerParams(vmem_limit_bytes=VMEM_LIMIT),
        name="sorted",
    )(targets, master, second)


def turned_kernel(*refs):
    parts, outs, sems = refs[:CROSS], refs[CROSS:-1], refs[-1]
    copies = [
        pltpu.make_async_copy(parts[i].at[1 + j], out.at[i], sems.at[j, i])
        for j, out in enumerate(outs[1:])
        for i in range(CROSS)
    ]
    for copy in copies:
        copy.start()
    for i in range(CROSS):
        outs[0][i] = parts[i][0]
    for copy in copies:
        copy.wait()


def turned(parts):
    ring, rows, lanes = parts[0].shape
    block = (CROSS, rows, lanes)
    return pl.pallas_call(
        turned_kernel,
        in_specs=[pl.BlockSpec(memory_space=pltpu.VMEM)] * CROSS,
        out_specs=[pl.BlockSpec(memory_space=pltpu.VMEM)] + [pl.BlockSpec(memory_space=pltpu.HBM)] * (ring - 1),
        out_shape=[pltpu.VMEM(block, jnp.bfloat16)] + [pltpu.HBM(block, jnp.bfloat16)] * (ring - 1),
        scratch_shapes=[pltpu.SemaphoreType.DMA((ring - 1, CROSS))],
        compiler_params=pltpu.CompilerParams(vmem_limit_bytes=VMEM_LIMIT),
        name="turned",
    )(*[pltpu.with_memory_space_constraint(part, pltpu.VMEM) for part in parts])


def row_total(parts):
    total = jnp.zeros(parts[0]().shape, jnp.float32)
    for part in parts:
        part = part().astype(jnp.float32)
        total = total + part * part
    return total


def inverse_scale(total):
    return jnp.broadcast_to(1.0 / jnp.sqrt(jnp.sum(total, axis=1, keepdims=True)), total.shape)


def first_kernel(parts_ref, out_ref, total_ref, out_vmem, sems):
    shards, _, lanes = parts_ref.shape
    experts, rows, _ = total_ref.shape
    blocks = rows // NORM_ROWS

    def copy(expert, block):
        at = (expert, pl.ds(block * NORM_ROWS, NORM_ROWS))
        return pltpu.make_async_copy(out_vmem.at[at], out_ref.at[at], sems.at[expert * blocks + block])

    for expert in range(experts):
        for block in range(blocks):
            at = pl.ds(block * NORM_ROWS, NORM_ROWS)
            taken = pl.ds(expert * rows + block * NORM_ROWS, NORM_ROWS)
            total = row_total([lambda s=s: parts_ref[s, taken] for s in range(shards)])
            total_ref[expert, at] = total
            inverse = inverse_scale(total)
            for s in range(shards):
                part = parts_ref[s, taken].astype(jnp.float32)
                out_vmem[expert, at, pl.ds(s * lanes, lanes)] = (part * inverse).astype(jnp.bfloat16)
            copy(expert, block).start()
    for expert in range(experts):
        for block in range(blocks):
            copy(expert, block).wait()


def first_normed(parts, experts, rows, full_rows):
    shards, _, lanes = parts.shape
    width = shards * lanes
    return pl.pallas_call(
        first_kernel,
        in_specs=[pl.BlockSpec(memory_space=pltpu.VMEM)],
        out_specs=[pl.BlockSpec(memory_space=pltpu.HBM), pl.BlockSpec(memory_space=pltpu.VMEM)],
        out_shape=[
            pltpu.HBM((experts, full_rows, width), jnp.bfloat16),
            pltpu.VMEM((experts, rows, lanes), jnp.float32),
        ],
        scratch_shapes=[
            pltpu.VMEM((experts, rows, width), jnp.bfloat16),
            pltpu.SemaphoreType.DMA((experts * rows // NORM_ROWS,)),
        ],
        compiler_params=pltpu.CompilerParams(vmem_limit_bytes=VMEM_LIMIT),
        name="first",
    )(pltpu.with_memory_space_constraint(parts, pltpu.VMEM))


def router_kernel(parts_ref, out_ref, router_vmem, sems):
    shards, rows, lanes = parts_ref.shape
    for s in range(shards):
        router_vmem[:, pl.ds(s * lanes, lanes)] = parts_ref[s, pl.ds(rows - TILE, TILE)][:router_vmem.shape[0]]
    copies = [pltpu.make_async_copy(router_vmem, out_ref.at[i], sems.at[i]) for i in range(out_ref.shape[0])]
    for copy in copies:
        copy.start()
    for copy in copies:
        copy.wait()


def router_copies(parts, columns, count):
    shards, _, lanes = parts.shape
    return pl.pallas_call(
        router_kernel,
        in_specs=[pl.BlockSpec(memory_space=pltpu.VMEM)],
        out_specs=pl.BlockSpec(memory_space=pltpu.HBM),
        out_shape=pltpu.HBM((count, columns, shards * lanes), jnp.bfloat16),
        scratch_shapes=[
            pltpu.VMEM((columns, shards * lanes), jnp.bfloat16),
            pltpu.SemaphoreType.DMA((count,)),
        ],
        compiler_params=pltpu.CompilerParams(vmem_limit_bytes=VMEM_LIMIT),
        name="router",
    )(pltpu.with_memory_space_constraint(parts, pltpu.VMEM))


def last_kernel(first_ref, *refs):
    parts = refs[:RING]
    out_ref, scale_ref, out_vmem, total_vmem, scale_vmem, sems, scale_sem = refs[RING + 1:]
    experts, rows, _ = out_vmem.shape
    first, lanes = first_ref.shape[1:]

    me = lax.axis_index("shard")
    z, c = me >> 2, me & (CROSS - 1)

    def column(j, i):
        place = (((z - j) & (RING - 1)) << 2) | ((c - i) & (CROSS - 1))
        return pl.ds(pl.multiple_of(place * lanes, lanes), lanes)

    def copy(expert):
        return pltpu.make_async_copy(out_vmem.at[expert], out_ref.at[expert, pl.ds(first, rows)], sems.at[expert])

    scale_copy = pltpu.make_async_copy(scale_vmem, scale_ref, scale_sem)
    for expert in range(experts):
        at = pl.ds(expert * rows, rows)
        total = row_total([lambda j=j, i=i: parts[j][i, at] for j in range(RING) for i in range(CROSS)])
        total_vmem[expert, pl.ds(0, first)] = first_ref[expert]
        total_vmem[expert, pl.ds(first, rows)] = total
        inverse = inverse_scale(total)
        for j in range(RING):
            for i in range(CROSS):
                part = parts[j][i, at].astype(jnp.float32)
                out_vmem[expert, :, column(j, i)] = (part * inverse).astype(jnp.bfloat16)
        copy(expert).start()
    for expert in range(experts):
        scale_vmem[pl.ds(expert, 1)] = jnp.sqrt(jnp.sum(jnp.transpose(total_vmem[expert]), axis=0, keepdims=True))
    scale_copy.start()
    for expert in range(experts):
        copy(expert).wait()
    scale_copy.wait()


def last_normed(totals, parts, final):
    experts, full_rows, width = final.shape
    rows, lanes = full_rows - totals.shape[1], totals.shape[2]
    return pl.pallas_call(
        last_kernel,
        in_specs=[pl.BlockSpec(memory_space=pltpu.VMEM)] * (1 + RING)
        + [pl.BlockSpec(memory_space=pltpu.HBM)],
        out_specs=[pl.BlockSpec(memory_space=pltpu.HBM)] * 2,
        out_shape=[
            pltpu.HBM(final.shape, jnp.bfloat16),
            pltpu.HBM((experts, full_rows), jnp.float32),
        ],
        scratch_shapes=[
            pltpu.VMEM((experts, rows, width), jnp.bfloat16),
            pltpu.VMEM((experts, full_rows, lanes), jnp.float32),
            pltpu.VMEM((experts, full_rows), jnp.float32),
            pltpu.SemaphoreType.DMA((experts,)),
            pltpu.SemaphoreType.DMA,
        ],
        input_output_aliases={1 + RING: 0},
        compiler_params=pltpu.CompilerParams(vmem_limit_bytes=VMEM_LIMIT),
        name="last",
    )(*[pltpu.with_memory_space_constraint(x, pltpu.VMEM) for x in (totals, *parts)], final)


def moved(x, dz, dx):
    pairs = [
        (z * CROSS + c, ((z + dz) % RING) * CROSS + (c + dx) % CROSS) for z in range(RING) for c in range(CROSS)
    ]
    return lax.ppermute(x, "shard", pairs)


def body(master_down, second_down, router_weight, router_gain):
    shards = lax.axis_size("shard")
    experts, rows, lanes = master_down.shape
    rows = rows // shards
    cut = (experts, shards, rows, lanes)
    master = pltpu.with_memory_space_constraint(master_down.reshape(cut), pltpu.HBM)
    second = pltpu.with_memory_space_constraint(second_down.reshape(cut), pltpu.HBM)
    me = lax.axis_index("shard")
    z, c = me >> 2, me & (CROSS - 1)
    steps = jnp.arange(shards, dtype=jnp.int32)
    targets = (((z + (steps & (RING - 1))) & (RING - 1)) << 2) | ((c + (steps >> 3)) & (CROSS - 1))
    sent = packed(master, second, router_weight.T, router_gain[None], FIRST_ROWS)
    received = lax.all_to_all(sent, "shard", 0, 0, tiled=True)
    parts = list(sorted_by_cross(targets, master, second, rows - FIRST_ROWS))
    for step in range(1, CROSS):
        parts[step] = moved(parts[step], 0, step)
    blocks = list(turned(parts))
    for step in ALONG:
        blocks[step] = moved(blocks[step], step, 0)
    copies = router_copies(received, router_weight.shape[1], lax.axis_size("expert"))
    gathered = lax.all_to_all(copies, "expert", 0, 0, tiled=True)
    final_down, totals = first_normed(received, experts, FIRST_ROWS, rows)
    serve_router = gathered.reshape(-1, shards * lanes)
    final_down, scale_down = last_normed(totals, blocks, final_down)
    return (final_down, scale_down, serve_router.T)


def solution(mesh):
    placed = (
        P("expert", None, "shard"),
        P("expert", None, "shard"),
        P("shard", "expert"),
        P("shard"),
    )
    return jax.shard_map(
        body,
        mesh=mesh,
        in_specs=placed,
        out_specs=(P("expert", "shard", None), P("expert", "shard"), P()),
        check_vma=False,
    )
```

```python
import jax
import jax.numpy as jnp
from jax import lax
from jax.experimental import pallas as pl
from jax.experimental.pallas import tpu as pltpu
from jax.sharding import PartitionSpec as P


RING, CROSS = 8, 4
FIRST_ROWS = 128
PACK_GROUPS = (16, 8, 4, 4)
NORM_ROWS = 32
VMEM_LIMIT = 32 << 20
ALONG = (4, 3, 5, 2, 6, 1, 7)


def merged(master, second):
    return (master + second.astype(jnp.float32)).astype(jnp.bfloat16)


def packed_kernel(master_ref, second_ref, out_ref, master_vmem, second_vmem, out_vmem, master_sem, second_sem, out_sem):
    rows = out_ref.shape[2]
    steps = len(PACK_GROUPS)

    def at(step):
        return pl.ds(sum(PACK_GROUPS[:step]), PACK_GROUPS[step])

    def copies(step):
        taken = (slice(None), at(step), pl.ds(0, rows))
        return (
            pltpu.make_async_copy(master_ref.at[taken], master_vmem.at[:, at(step)], master_sem.at[step]),
            pltpu.make_async_copy(second_ref.at[taken], second_vmem.at[:, at(step)], second_sem.at[step]),
        )

    def copy_out(step):
        return pltpu.make_async_copy(out_vmem.at[at(step)], out_ref.at[at(step)], out_sem.at[step])

    for step in range(steps):
        for copy in copies(step):
            copy.start()
    for step in range(steps):
        for copy in copies(step):
            copy.wait()
        for s in range(sum(PACK_GROUPS[:step]), sum(PACK_GROUPS[:step + 1])):
            out_vmem[s] = merged(master_vmem[:, s], second_vmem[:, s])
        copy_out(step).start()
    for step in range(steps):
        copy_out(step).wait()


def packed(master, second, rows):
    experts, shards, _, lanes = master.shape
    steps = len(PACK_GROUPS)
    return pl.pallas_call(
        packed_kernel,
        in_specs=[pl.BlockSpec(memory_space=pltpu.HBM)] * 2,
        out_specs=pl.BlockSpec(memory_space=pltpu.HBM),
        out_shape=pltpu.HBM((shards, experts, rows, lanes), jnp.bfloat16),
        scratch_shapes=[
            pltpu.VMEM((experts, shards, rows, lanes), jnp.float32),
            pltpu.VMEM((experts, shards, rows, lanes), jnp.bfloat16),
            pltpu.VMEM((shards, experts, rows, lanes), jnp.bfloat16),
            pltpu.SemaphoreType.DMA((steps,)),
            pltpu.SemaphoreType.DMA((steps,)),
            pltpu.SemaphoreType.DMA((steps,)),
        ],
        compiler_params=pltpu.CompilerParams(vmem_limit_bytes=VMEM_LIMIT),
        name="packed",
    )(master, second)


def sorted_kernel(targets, master_ref, second_ref, *refs):
    outs = refs[:CROSS]
    master_vmem, second_vmem, out_vmem, master_sem, second_sem, out_sem = refs[CROSS:]
    experts, shards, rows, _ = master_vmem.shape
    first = master_ref.shape[2] - rows

    def copies(s):
        taken = (slice(None), targets[s], pl.ds(first, rows))
        return (
            pltpu.make_async_copy(master_ref.at[taken], master_vmem.at[:, s], master_sem.at[s]),
            pltpu.make_async_copy(second_ref.at[taken], second_vmem.at[:, s], second_sem.at[s]),
        )

    def copy_out(i):
        return pltpu.make_async_copy(out_vmem.at[i], outs[i], out_sem.at[i])

    for s in range(shards):
        for copy in copies(s):
            copy.start()
    for i in range(CROSS):
        for j in range(RING):
            for copy in copies(i * RING + j):
                copy.wait()
            for expert in range(experts):
                out_vmem[i, j, pl.ds(expert * rows, rows)] = merged(
                    master_vmem[expert, i * RING + j], second_vmem[expert, i * RING + j]
                )
        copy_out(i).start()
    for i in range(CROSS):
        copy_out(i).wait()


def sorted_by_cross(targets, master, second, rows):
    experts, shards, _, lanes = master.shape
    block = (RING, experts * rows, lanes)
    return pl.pallas_call(
        sorted_kernel,
        in_specs=[pl.BlockSpec(memory_space=pltpu.SMEM)] + [pl.BlockSpec(memory_space=pltpu.HBM)] * 2,
        out_specs=[pl.BlockSpec(memory_space=pltpu.HBM)] * CROSS,
        out_shape=[pltpu.HBM(block, jnp.bfloat16)] * CROSS,
        scratch_shapes=[
            pltpu.VMEM((experts, shards, rows, lanes), jnp.float32),
            pltpu.VMEM((experts, shards, rows, lanes), jnp.bfloat16),
            pltpu.VMEM((CROSS, *block), jnp.bfloat16),
            pltpu.SemaphoreType.DMA((shards,)),
            pltpu.SemaphoreType.DMA((shards,)),
            pltpu.SemaphoreType.DMA((CROSS,)),
        ],
        compiler_params=pltpu.CompilerParams(vmem_limit_bytes=VMEM_LIMIT),
        name="sorted",
    )(targets, master, second)


def turned_kernel(*refs):
    parts, outs, sems = refs[:CROSS], refs[CROSS:-1], refs[-1]
    copies = [
        pltpu.make_async_copy(parts[i].at[1 + j], out.at[i], sems.at[j, i])
        for j, out in enumerate(outs[1:])
        for i in range(CROSS)
    ]
    for copy in copies:
        copy.start()
    for i in range(CROSS):
        outs[0][i] = parts[i][0]
    for copy in copies:
        copy.wait()


def turned(parts):
    ring, rows, lanes = parts[0].shape
    block = (CROSS, rows, lanes)
    return pl.pallas_call(
        turned_kernel,
        in_specs=[pl.BlockSpec(memory_space=pltpu.VMEM)] * CROSS,
        out_specs=[pl.BlockSpec(memory_space=pltpu.VMEM)] + [pl.BlockSpec(memory_space=pltpu.HBM)] * (ring - 1),
        out_shape=[pltpu.VMEM(block, jnp.bfloat16)] + [pltpu.HBM(block, jnp.bfloat16)] * (ring - 1),
        scratch_shapes=[pltpu.SemaphoreType.DMA((ring - 1, CROSS))],
        compiler_params=pltpu.CompilerParams(vmem_limit_bytes=VMEM_LIMIT),
        name="turned",
    )(*[pltpu.with_memory_space_constraint(part, pltpu.VMEM) for part in parts])


def row_total(parts):
    total = jnp.zeros(parts[0]().shape, jnp.float32)
    for part in parts:
        part = part().astype(jnp.float32)
        total = total + part * part
    return total


def inverse_scale(total):
    return jnp.broadcast_to(1.0 / jnp.sqrt(jnp.sum(total, axis=1, keepdims=True)), total.shape)


def first_kernel(parts_ref, out_ref, total_ref, out_vmem, sems):
    shards, experts, rows, lanes = parts_ref.shape
    blocks = rows // NORM_ROWS

    def copy(expert, block):
        at = (expert, pl.ds(block * NORM_ROWS, NORM_ROWS))
        return pltpu.make_async_copy(out_vmem.at[at], out_ref.at[at], sems.at[expert * blocks + block])

    for expert in range(experts):
        for block in range(blocks):
            at = pl.ds(block * NORM_ROWS, NORM_ROWS)
            total = row_total([lambda s=s: parts_ref[s, expert, at] for s in range(shards)])
            total_ref[expert, at] = total
            inverse = inverse_scale(total)
            for s in range(shards):
                part = parts_ref[s, expert, at].astype(jnp.float32)
                out_vmem[expert, at, pl.ds(s * lanes, lanes)] = (part * inverse).astype(jnp.bfloat16)
            copy(expert, block).start()
    for expert in range(experts):
        for block in range(blocks):
            copy(expert, block).wait()


def first_normed(parts, full_rows):
    shards, experts, rows, lanes = parts.shape
    width = shards * lanes
    return pl.pallas_call(
        first_kernel,
        in_specs=[pl.BlockSpec(memory_space=pltpu.VMEM)],
        out_specs=[pl.BlockSpec(memory_space=pltpu.HBM), pl.BlockSpec(memory_space=pltpu.VMEM)],
        out_shape=[
            pltpu.HBM((experts, full_rows, width), jnp.bfloat16),
            pltpu.VMEM((experts, rows, lanes), jnp.float32),
        ],
        scratch_shapes=[
            pltpu.VMEM((experts, rows, width), jnp.bfloat16),
            pltpu.SemaphoreType.DMA((experts * rows // NORM_ROWS,)),
        ],
        compiler_params=pltpu.CompilerParams(vmem_limit_bytes=VMEM_LIMIT),
        name="first",
    )(pltpu.with_memory_space_constraint(parts, pltpu.VMEM))


def column_at(j, i, lanes):
    me = lax.axis_index("shard")
    z, c = me >> 2, me & (CROSS - 1)
    place = (((z - j) & (RING - 1)) << 2) | ((c - i) & (CROSS - 1))
    return pl.ds(pl.multiple_of(place * lanes, lanes), lanes)


def router_kernel(*refs):
    tiles, (out_ref, router_vmem, sems) = refs[:RING], refs[RING:]
    columns = router_vmem.shape[0]
    lanes = tiles[0].shape[1]
    for j in range(RING):
        tile = tiles[j][...]
        for i in range(CROSS):
            router_vmem[:, column_at(j, i, lanes)] = tile[i * columns:(i + 1) * columns]
    copies = [pltpu.make_async_copy(router_vmem, out_ref.at[i], sems.at[i]) for i in range(out_ref.shape[0])]
    for copy in copies:
        copy.start()
    for copy in copies:
        copy.wait()


def router_copies(tiles, count):
    columns, lanes = tiles[0].shape[0] // CROSS, tiles[0].shape[1]
    width = RING * CROSS * lanes
    return pl.pallas_call(
        router_kernel,
        in_specs=[pl.BlockSpec(memory_space=pltpu.VMEM)] * RING,
        out_specs=pl.BlockSpec(memory_space=pltpu.HBM),
        out_shape=pltpu.HBM((count, columns, width), jnp.bfloat16),
        scratch_shapes=[
            pltpu.VMEM((columns, width), jnp.bfloat16),
            pltpu.SemaphoreType.DMA((count,)),
        ],
        compiler_params=pltpu.CompilerParams(vmem_limit_bytes=VMEM_LIMIT),
        name="router",
    )(*[pltpu.with_memory_space_constraint(tile, pltpu.VMEM) for tile in tiles])


def last_kernel(first_ref, *refs):
    parts = refs[:RING]
    out_ref, scale_ref, out_vmem, total_vmem, scale_vmem, sems, scale_sem = refs[RING + 1:]
    experts, rows, _ = out_vmem.shape
    first, lanes = first_ref.shape[1:]

    def column(j, i):
        return column_at(j, i, lanes)

    def copy(expert):
        return pltpu.make_async_copy(out_vmem.at[expert], out_ref.at[expert, pl.ds(first, rows)], sems.at[expert])

    scale_copy = pltpu.make_async_copy(scale_vmem, scale_ref, scale_sem)
    for expert in range(experts):
        at = pl.ds(expert * rows, rows)
        total = row_total([lambda j=j, i=i: parts[j][i, at] for j in range(RING) for i in range(CROSS)])
        total_vmem[expert, pl.ds(0, first)] = first_ref[expert]
        total_vmem[expert, pl.ds(first, rows)] = total
        inverse = inverse_scale(total)
        for j in range(RING):
            for i in range(CROSS):
                part = parts[j][i, at].astype(jnp.float32)
                out_vmem[expert, :, column(j, i)] = (part * inverse).astype(jnp.bfloat16)
        copy(expert).start()
    for expert in range(experts):
        scale_vmem[pl.ds(expert, 1)] = jnp.sqrt(jnp.sum(jnp.transpose(total_vmem[expert]), axis=0, keepdims=True))
    scale_copy.start()
    for expert in range(experts):
        copy(expert).wait()
    scale_copy.wait()


def last_normed(totals, parts, final):
    experts, full_rows, width = final.shape
    rows, lanes = full_rows - totals.shape[1], totals.shape[2]
    return pl.pallas_call(
        last_kernel,
        in_specs=[pl.BlockSpec(memory_space=pltpu.VMEM)] * (1 + RING)
        + [pl.BlockSpec(memory_space=pltpu.HBM)],
        out_specs=[pl.BlockSpec(memory_space=pltpu.HBM)] * 2,
        out_shape=[
            pltpu.HBM(final.shape, jnp.bfloat16),
            pltpu.HBM((experts, full_rows), jnp.float32),
        ],
        scratch_shapes=[
            pltpu.VMEM((experts, rows, width), jnp.bfloat16),
            pltpu.VMEM((experts, full_rows, lanes), jnp.float32),
            pltpu.VMEM((experts, full_rows), jnp.float32),
            pltpu.SemaphoreType.DMA((experts,)),
            pltpu.SemaphoreType.DMA,
        ],
        input_output_aliases={1 + RING: 0},
        compiler_params=pltpu.CompilerParams(vmem_limit_bytes=VMEM_LIMIT),
        name="last",
    )(*[pltpu.with_memory_space_constraint(x, pltpu.VMEM) for x in (totals, *parts)], final)


def moved(x, dz, dx):
    pairs = [
        (z * CROSS + c, ((z + dz) % RING) * CROSS + (c + dx) % CROSS) for z in range(RING) for c in range(CROSS)
    ]
    return lax.ppermute(x, "shard", pairs)


def body(master_down, second_down, router_weight, router_gain):
    shards = lax.axis_size("shard")
    experts, rows, lanes = master_down.shape
    rows = rows // shards
    cut = (experts, shards, rows, lanes)
    master = pltpu.with_memory_space_constraint(master_down.reshape(cut), pltpu.HBM)
    second = pltpu.with_memory_space_constraint(second_down.reshape(cut), pltpu.HBM)
    me = lax.axis_index("shard")
    z, c = me >> 2, me & (CROSS - 1)
    steps = jnp.arange(shards, dtype=jnp.int32)
    targets = (((z + (steps & (RING - 1))) & (RING - 1)) << 2) | ((c + (steps >> 3)) & (CROSS - 1))
    sent = packed(master, second, FIRST_ROWS)
    received = lax.all_to_all(sent, "shard", 0, 0, tiled=True)
    pieces = [(router_weight * router_gain[:, None]).astype(jnp.bfloat16).T]
    for step in range(1, CROSS):
        pieces.append(moved(pieces[0], 0, step))
    tile = jnp.concatenate(pieces, axis=0)
    tiles = [tile] * RING
    for step in ALONG:
        tiles[step] = moved(tile, step, 0)
    parts = list(sorted_by_cross(targets, master, second, rows - FIRST_ROWS))
    for step in range(1, CROSS):
        parts[step] = moved(parts[step], 0, step)
    blocks = list(turned(parts))
    for step in ALONG:
        blocks[step] = moved(blocks[step], step, 0)
    copies = router_copies(tiles, lax.axis_size("expert"))
    gathered = lax.all_to_all(copies, "expert", 0, 0, tiled=True)
    final_down, totals = first_normed(received, rows)
    serve_router = gathered.reshape(-1, shards * lanes)
    final_down, scale_down = last_normed(totals, blocks, final_down)
    return (final_down, scale_down, serve_router.T)


def solution(mesh):
    placed = (
        P("expert", None, "shard"),
        P("expert", None, "shard"),
        P("shard", "expert"),
        P("shard"),
    )
    return jax.shard_map(
        body,
        mesh=mesh,
        in_specs=placed,
        out_specs=(P("expert", "shard", None), P("expert", "shard"), P()),
        check_vma=False,
    )
```

```python
import jax
import jax.numpy as jnp
from jax import lax
from jax.experimental import pallas as pl
from jax.experimental.pallas import tpu as pltpu
from jax.sharding import PartitionSpec as P


RING, CROSS = 8, 4
LAST_CUT = 40
FIRST_ROWS = 128
PACK_GROUPS = (16, 8, 4, 4)
NORM_ROWS = 32
VMEM_LIMIT = 32 << 20
ALONG = (4, 3, 5, 2, 6, 1, 7)


def merged(master, second):
    return (master + second.astype(jnp.float32)).astype(jnp.bfloat16)


def packed_kernel(master_ref, second_ref, out_ref, master_vmem, second_vmem, out_vmem, master_sem, second_sem, out_sem):
    rows = out_ref.shape[2]
    steps = len(PACK_GROUPS)

    def at(step):
        return pl.ds(sum(PACK_GROUPS[:step]), PACK_GROUPS[step])

    def copies(step):
        taken = (slice(None), at(step), pl.ds(0, rows))
        return (
            pltpu.make_async_copy(master_ref.at[taken], master_vmem.at[:, at(step)], master_sem.at[step]),
            pltpu.make_async_copy(second_ref.at[taken], second_vmem.at[:, at(step)], second_sem.at[step]),
        )

    def copy_out(step):
        return pltpu.make_async_copy(out_vmem.at[at(step)], out_ref.at[at(step)], out_sem.at[step])

    for step in range(steps):
        for copy in copies(step):
            copy.start()
    for step in range(steps):
        for copy in copies(step):
            copy.wait()
        for s in range(sum(PACK_GROUPS[:step]), sum(PACK_GROUPS[:step + 1])):
            out_vmem[s] = merged(master_vmem[:, s], second_vmem[:, s])
        copy_out(step).start()
    for step in range(steps):
        copy_out(step).wait()


def packed(master, second, rows):
    experts, shards, _, lanes = master.shape
    steps = len(PACK_GROUPS)
    return pl.pallas_call(
        packed_kernel,
        in_specs=[pl.BlockSpec(memory_space=pltpu.HBM)] * 2,
        out_specs=pl.BlockSpec(memory_space=pltpu.HBM),
        out_shape=pltpu.HBM((shards, experts, rows, lanes), jnp.bfloat16),
        scratch_shapes=[
            pltpu.VMEM((experts, shards, rows, lanes), jnp.float32),
            pltpu.VMEM((experts, shards, rows, lanes), jnp.bfloat16),
            pltpu.VMEM((shards, experts, rows, lanes), jnp.bfloat16),
            pltpu.SemaphoreType.DMA((steps,)),
            pltpu.SemaphoreType.DMA((steps,)),
            pltpu.SemaphoreType.DMA((steps,)),
        ],
        compiler_params=pltpu.CompilerParams(vmem_limit_bytes=VMEM_LIMIT),
        name="packed",
    )(master, second)


def sorted_kernel(targets, master_ref, second_ref, *refs):
    outs = refs[:CROSS]
    master_vmem, second_vmem, out_vmem, master_sem, second_sem, out_sem = refs[CROSS:]
    experts, shards, rows, _ = master_vmem.shape
    first = master_ref.shape[2] - rows

    def copies(s):
        taken = (slice(None), targets[s], pl.ds(first, rows))
        return (
            pltpu.make_async_copy(master_ref.at[taken], master_vmem.at[:, s], master_sem.at[s]),
            pltpu.make_async_copy(second_ref.at[taken], second_vmem.at[:, s], second_sem.at[s]),
        )

    def copy_out(i):
        return pltpu.make_async_copy(out_vmem.at[i], outs[i], out_sem.at[i])

    for s in range(shards):
        for copy in copies(s):
            copy.start()
    for i in range(CROSS):
        for j in range(RING):
            for copy in copies(i * RING + j):
                copy.wait()
            for expert in range(experts):
                out_vmem[i, j, pl.ds(expert * rows, rows)] = merged(
                    master_vmem[expert, i * RING + j], second_vmem[expert, i * RING + j]
                )
        copy_out(i).start()
    for i in range(CROSS):
        copy_out(i).wait()


def sorted_by_cross(targets, master, second, rows):
    experts, shards, _, lanes = master.shape
    block = (RING, experts * rows, lanes)
    return pl.pallas_call(
        sorted_kernel,
        in_specs=[pl.BlockSpec(memory_space=pltpu.SMEM)] + [pl.BlockSpec(memory_space=pltpu.HBM)] * 2,
        out_specs=[pl.BlockSpec(memory_space=pltpu.HBM)] * CROSS,
        out_shape=[pltpu.HBM(block, jnp.bfloat16)] * CROSS,
        scratch_shapes=[
            pltpu.VMEM((experts, shards, rows, lanes), jnp.float32),
            pltpu.VMEM((experts, shards, rows, lanes), jnp.bfloat16),
            pltpu.VMEM((CROSS, *block), jnp.bfloat16),
            pltpu.SemaphoreType.DMA((shards,)),
            pltpu.SemaphoreType.DMA((shards,)),
            pltpu.SemaphoreType.DMA((CROSS,)),
        ],
        compiler_params=pltpu.CompilerParams(vmem_limit_bytes=VMEM_LIMIT),
        name="sorted",
    )(targets, master, second)


def turned_kernel(*refs):
    parts, outs, sems = refs[:CROSS], refs[CROSS:-1], refs[-1]
    copies = [
        pltpu.make_async_copy(parts[i].at[1 + j], out.at[i], sems.at[j, i])
        for j, out in enumerate(outs[1:])
        for i in range(CROSS)
    ]
    for copy in copies:
        copy.start()
    for i in range(CROSS):
        outs[0][i] = parts[i][0]
    for copy in copies:
        copy.wait()


def turned(parts):
    ring, rows, lanes = parts[0].shape
    block = (CROSS, rows, lanes)
    return pl.pallas_call(
        turned_kernel,
        in_specs=[pl.BlockSpec(memory_space=pltpu.VMEM)] * CROSS,
        out_specs=[pl.BlockSpec(memory_space=pltpu.VMEM)] + [pl.BlockSpec(memory_space=pltpu.HBM)] * (ring - 1),
        out_shape=[pltpu.VMEM(block, jnp.bfloat16)] + [pltpu.HBM(block, jnp.bfloat16)] * (ring - 1),
        scratch_shapes=[pltpu.SemaphoreType.DMA((ring - 1, CROSS))],
        compiler_params=pltpu.CompilerParams(vmem_limit_bytes=VMEM_LIMIT),
        name="turned",
    )(*[pltpu.with_memory_space_constraint(part, pltpu.VMEM) for part in parts])


def row_total(parts):
    total = jnp.zeros(parts[0]().shape, jnp.float32)
    for part in parts:
        part = part().astype(jnp.float32)
        total = total + part * part
    return total


def inverse_scale(total):
    return jnp.broadcast_to(1.0 / jnp.sqrt(jnp.sum(total, axis=1, keepdims=True)), total.shape)


def first_kernel(parts_ref, out_ref, total_ref, out_vmem, sems):
    shards, experts, rows, lanes = parts_ref.shape
    blocks = rows // NORM_ROWS

    def copy(expert, block):
        at = (expert, pl.ds(block * NORM_ROWS, NORM_ROWS))
        return pltpu.make_async_copy(out_vmem.at[at], out_ref.at[at], sems.at[expert * blocks + block])

    for expert in range(experts):
        for block in range(blocks):
            at = pl.ds(block * NORM_ROWS, NORM_ROWS)
            total = row_total([lambda s=s: parts_ref[s, expert, at] for s in range(shards)])
            total_ref[expert, at] = total
            inverse = inverse_scale(total)
            for s in range(shards):
                part = parts_ref[s, expert, at].astype(jnp.float32)
                out_vmem[expert, at, pl.ds(s * lanes, lanes)] = (part * inverse).astype(jnp.bfloat16)
            copy(expert, block).start()
    for expert in range(experts):
        for block in range(blocks):
            copy(expert, block).wait()


def first_normed(parts, full_rows):
    shards, experts, rows, lanes = parts.shape
    width = shards * lanes
    return pl.pallas_call(
        first_kernel,
        in_specs=[pl.BlockSpec(memory_space=pltpu.VMEM)],
        out_specs=[pl.BlockSpec(memory_space=pltpu.HBM), pl.BlockSpec(memory_space=pltpu.VMEM)],
        out_shape=[
            pltpu.HBM((experts, full_rows, width), jnp.bfloat16),
            pltpu.VMEM((experts, rows, lanes), jnp.float32),
        ],
        scratch_shapes=[
            pltpu.VMEM((experts, rows, width), jnp.bfloat16),
            pltpu.SemaphoreType.DMA((experts * rows // NORM_ROWS,)),
        ],
        compiler_params=pltpu.CompilerParams(vmem_limit_bytes=VMEM_LIMIT),
        name="first",
    )(pltpu.with_memory_space_constraint(parts, pltpu.VMEM))


def column_at(j, i, lanes):
    me = lax.axis_index("shard")
    z, c = me >> 2, me & (CROSS - 1)
    place = (((z - j) & (RING - 1)) << 2) | ((c - i) & (CROSS - 1))
    return pl.ds(pl.multiple_of(place * lanes, lanes), lanes)


def router_kernel(*refs):
    tiles, (out_ref, router_vmem, sems) = refs[:RING], refs[RING:]
    columns = router_vmem.shape[0]
    lanes = tiles[0].shape[1]
    for j in range(RING):
        tile = tiles[j][...]
        for i in range(CROSS):
            router_vmem[:, column_at(j, i, lanes)] = tile[i * columns:(i + 1) * columns]
    copies = [pltpu.make_async_copy(router_vmem, out_ref.at[i], sems.at[i]) for i in range(out_ref.shape[0])]
    for copy in copies:
        copy.start()
    for copy in copies:
        copy.wait()


def router_copies(tiles, count):
    columns, lanes = tiles[0].shape[0] // CROSS, tiles[0].shape[1]
    width = RING * CROSS * lanes
    return pl.pallas_call(
        router_kernel,
        in_specs=[pl.BlockSpec(memory_space=pltpu.VMEM)] * RING,
        out_specs=pl.BlockSpec(memory_space=pltpu.HBM),
        out_shape=pltpu.HBM((count, columns, width), jnp.bfloat16),
        scratch_shapes=[
            pltpu.VMEM((columns, width), jnp.bfloat16),
            pltpu.SemaphoreType.DMA((count,)),
        ],
        compiler_params=pltpu.CompilerParams(vmem_limit_bytes=VMEM_LIMIT),
        name="router",
    )(*[pltpu.with_memory_space_constraint(tile, pltpu.VMEM) for tile in tiles])


def last_kernel(first_ref, *refs):
    parts = refs[:RING]
    out_ref, scale_ref, out_vmem, total_vmem, scale_vmem, sems, scale_sem = refs[RING + 1:]
    experts, rows, _ = out_vmem.shape
    first, lanes = first_ref.shape[1:]
    cuts = ((0, LAST_CUT), (LAST_CUT, rows - LAST_CUT))

    def column(j, i):
        return column_at(j, i, lanes)

    def copy(expert, k):
        start, size = cuts[k]
        return pltpu.make_async_copy(
            out_vmem.at[expert, pl.ds(start, size)], out_ref.at[expert, pl.ds(first + start, size)], sems.at[expert, k]
        )

    scale_copy = pltpu.make_async_copy(scale_vmem, scale_ref, scale_sem)
    for expert in range(experts):
        total_vmem[expert, pl.ds(0, first)] = first_ref[expert]
        for k, (start, size) in enumerate(cuts):
            at = pl.ds(expert * rows + start, size)
            total = row_total([lambda j=j, i=i: parts[j][i, at] for j in range(RING) for i in range(CROSS)])
            total_vmem[expert, pl.ds(first + start, size)] = total
            inverse = inverse_scale(total)
            for j in range(RING):
                for i in range(CROSS):
                    part = parts[j][i, at].astype(jnp.float32)
                    out_vmem[expert, pl.ds(start, size), column(j, i)] = (part * inverse).astype(jnp.bfloat16)
            copy(expert, k).start()
    for expert in range(experts):
        scale_vmem[pl.ds(expert, 1)] = jnp.sqrt(jnp.sum(jnp.transpose(total_vmem[expert]), axis=0, keepdims=True))
    scale_copy.start()
    for expert in range(experts):
        for k in range(len(cuts)):
            copy(expert, k).wait()
    scale_copy.wait()


def last_normed(totals, parts, final):
    experts, full_rows, width = final.shape
    rows, lanes = full_rows - totals.shape[1], totals.shape[2]
    return pl.pallas_call(
        last_kernel,
        in_specs=[pl.BlockSpec(memory_space=pltpu.VMEM)] * (1 + RING)
        + [pl.BlockSpec(memory_space=pltpu.HBM)],
        out_specs=[pl.BlockSpec(memory_space=pltpu.HBM)] * 2,
        out_shape=[
            pltpu.HBM(final.shape, jnp.bfloat16),
            pltpu.HBM((experts, full_rows), jnp.float32),
        ],
        scratch_shapes=[
            pltpu.VMEM((experts, rows, width), jnp.bfloat16),
            pltpu.VMEM((experts, full_rows, lanes), jnp.float32),
            pltpu.VMEM((experts, full_rows), jnp.float32),
            pltpu.SemaphoreType.DMA((experts, 2)),
            pltpu.SemaphoreType.DMA,
        ],
        input_output_aliases={1 + RING: 0},
        compiler_params=pltpu.CompilerParams(vmem_limit_bytes=VMEM_LIMIT),
        name="last",
    )(*[pltpu.with_memory_space_constraint(x, pltpu.VMEM) for x in (totals, *parts)], final)


def moved(x, dz, dx):
    pairs = [
        (z * CROSS + c, ((z + dz) % RING) * CROSS + (c + dx) % CROSS) for z in range(RING) for c in range(CROSS)
    ]
    return lax.ppermute(x, "shard", pairs)


def body(master_down, second_down, router_weight, router_gain):
    shards = lax.axis_size("shard")
    experts, rows, lanes = master_down.shape
    rows = rows // shards
    cut = (experts, shards, rows, lanes)
    master = pltpu.with_memory_space_constraint(master_down.reshape(cut), pltpu.HBM)
    second = pltpu.with_memory_space_constraint(second_down.reshape(cut), pltpu.HBM)
    me = lax.axis_index("shard")
    z, c = me >> 2, me & (CROSS - 1)
    steps = jnp.arange(shards, dtype=jnp.int32)
    targets = (((z + (steps & (RING - 1))) & (RING - 1)) << 2) | ((c + (steps >> 3)) & (CROSS - 1))
    sent = packed(master, second, FIRST_ROWS)
    received = lax.all_to_all(sent, "shard", 0, 0, tiled=True)
    pieces = [(router_weight * router_gain[:, None]).astype(jnp.bfloat16).T]
    for step in range(1, CROSS):
        pieces.append(moved(pieces[0], 0, step))
    tile = jnp.concatenate(pieces, axis=0)
    tiles = [tile] * RING
    for step in ALONG:
        tiles[step] = moved(tile, step, 0)
    parts = list(sorted_by_cross(targets, master, second, rows - FIRST_ROWS))
    for step in range(1, CROSS):
        parts[step] = moved(parts[step], 0, step)
    blocks = list(turned(parts))
    for step in ALONG:
        blocks[step] = moved(blocks[step], step, 0)
    copies = router_copies(tiles, lax.axis_size("expert"))
    gathered = lax.all_to_all(copies, "expert", 0, 0, tiled=True)
    final_down, totals = first_normed(received, rows)
    serve_router = gathered.reshape(-1, shards * lanes)
    final_down, scale_down = last_normed(totals, blocks, final_down)
    return (final_down, scale_down, serve_router.T)


def solution(mesh):
    placed = (
        P("expert", None, "shard"),
        P("expert", None, "shard"),
        P("shard", "expert"),
        P("shard"),
    )
    return jax.shard_map(
        body,
        mesh=mesh,
        in_specs=placed,
        out_specs=(P("expert", "shard", None), P("expert", "shard"), P()),
        check_vma=False,
    )
```

```python
import jax
import jax.numpy as jnp
from jax import lax
from jax.experimental import pallas as pl
from jax.experimental.pallas import tpu as pltpu
from jax.sharding import PartitionSpec as P


RING, CROSS = 8, 4
LAST_CUT = 40
LATE = (1, 7)
FIRST_ROWS = 128
PACK_GROUPS = (16, 8, 4, 4)
NORM_ROWS = 32
VMEM_LIMIT = 32 << 20
ALONG = (4, 3, 5, 2, 6, 1, 7)


def merged(master, second):
    return (master + second.astype(jnp.float32)).astype(jnp.bfloat16)


def packed_kernel(master_ref, second_ref, out_ref, master_vmem, second_vmem, out_vmem, master_sem, second_sem, out_sem):
    rows = out_ref.shape[2]
    steps = len(PACK_GROUPS)

    def at(step):
        return pl.ds(sum(PACK_GROUPS[:step]), PACK_GROUPS[step])

    def copies(step):
        taken = (slice(None), at(step), pl.ds(0, rows))
        return (
            pltpu.make_async_copy(master_ref.at[taken], master_vmem.at[:, at(step)], master_sem.at[step]),
            pltpu.make_async_copy(second_ref.at[taken], second_vmem.at[:, at(step)], second_sem.at[step]),
        )

    def copy_out(step):
        return pltpu.make_async_copy(out_vmem.at[at(step)], out_ref.at[at(step)], out_sem.at[step])

    for step in range(steps):
        for copy in copies(step):
            copy.start()
    for step in range(steps):
        for copy in copies(step):
            copy.wait()
        for s in range(sum(PACK_GROUPS[:step]), sum(PACK_GROUPS[:step + 1])):
            out_vmem[s] = merged(master_vmem[:, s], second_vmem[:, s])
        copy_out(step).start()
    for step in range(steps):
        copy_out(step).wait()


def packed(master, second, rows):
    experts, shards, _, lanes = master.shape
    steps = len(PACK_GROUPS)
    return pl.pallas_call(
        packed_kernel,
        in_specs=[pl.BlockSpec(memory_space=pltpu.HBM)] * 2,
        out_specs=pl.BlockSpec(memory_space=pltpu.HBM),
        out_shape=pltpu.HBM((shards, experts, rows, lanes), jnp.bfloat16),
        scratch_shapes=[
            pltpu.VMEM((experts, shards, rows, lanes), jnp.float32),
            pltpu.VMEM((experts, shards, rows, lanes), jnp.bfloat16),
            pltpu.VMEM((shards, experts, rows, lanes), jnp.bfloat16),
            pltpu.SemaphoreType.DMA((steps,)),
            pltpu.SemaphoreType.DMA((steps,)),
            pltpu.SemaphoreType.DMA((steps,)),
        ],
        compiler_params=pltpu.CompilerParams(vmem_limit_bytes=VMEM_LIMIT),
        name="packed",
    )(master, second)


def sorted_kernel(targets, master_ref, second_ref, *refs):
    outs = refs[:CROSS]
    master_vmem, second_vmem, out_vmem, master_sem, second_sem, out_sem = refs[CROSS:]
    experts, shards, rows, _ = master_vmem.shape
    first = master_ref.shape[2] - rows

    def copies(s):
        taken = (slice(None), targets[s], pl.ds(first, rows))
        return (
            pltpu.make_async_copy(master_ref.at[taken], master_vmem.at[:, s], master_sem.at[s]),
            pltpu.make_async_copy(second_ref.at[taken], second_vmem.at[:, s], second_sem.at[s]),
        )

    def copy_out(i):
        return pltpu.make_async_copy(out_vmem.at[i], outs[i], out_sem.at[i])

    for s in range(shards):
        for copy in copies(s):
            copy.start()
    for i in range(CROSS):
        for j in range(RING):
            for copy in copies(i * RING + j):
                copy.wait()
            for expert in range(experts):
                out_vmem[i, j, pl.ds(expert * rows, rows)] = merged(
                    master_vmem[expert, i * RING + j], second_vmem[expert, i * RING + j]
                )
        copy_out(i).start()
    for i in range(CROSS):
        copy_out(i).wait()


def sorted_by_cross(targets, master, second, rows):
    experts, shards, _, lanes = master.shape
    block = (RING, experts * rows, lanes)
    return pl.pallas_call(
        sorted_kernel,
        in_specs=[pl.BlockSpec(memory_space=pltpu.SMEM)] + [pl.BlockSpec(memory_space=pltpu.HBM)] * 2,
        out_specs=[pl.BlockSpec(memory_space=pltpu.HBM)] * CROSS,
        out_shape=[pltpu.HBM(block, jnp.bfloat16)] * CROSS,
        scratch_shapes=[
            pltpu.VMEM((experts, shards, rows, lanes), jnp.float32),
            pltpu.VMEM((experts, shards, rows, lanes), jnp.bfloat16),
            pltpu.VMEM((CROSS, *block), jnp.bfloat16),
            pltpu.SemaphoreType.DMA((shards,)),
            pltpu.SemaphoreType.DMA((shards,)),
            pltpu.SemaphoreType.DMA((CROSS,)),
        ],
        compiler_params=pltpu.CompilerParams(vmem_limit_bytes=VMEM_LIMIT),
        name="sorted",
    )(targets, master, second)


def turned_kernel(*refs):
    parts, outs, sems = refs[:CROSS], refs[CROSS:-1], refs[-1]
    copies = [
        pltpu.make_async_copy(parts[i].at[1 + j], out.at[i], sems.at[j, i])
        for j, out in enumerate(outs[1:])
        for i in range(CROSS)
    ]
    for copy in copies:
        copy.start()
    for i in range(CROSS):
        outs[0][i] = parts[i][0]
    for copy in copies:
        copy.wait()


def turned(parts):
    ring, rows, lanes = parts[0].shape
    block = (CROSS, rows, lanes)
    return pl.pallas_call(
        turned_kernel,
        in_specs=[pl.BlockSpec(memory_space=pltpu.VMEM)] * CROSS,
        out_specs=[pl.BlockSpec(memory_space=pltpu.VMEM)] + [pl.BlockSpec(memory_space=pltpu.HBM)] * (ring - 1),
        out_shape=[pltpu.VMEM(block, jnp.bfloat16)] + [pltpu.HBM(block, jnp.bfloat16)] * (ring - 1),
        scratch_shapes=[pltpu.SemaphoreType.DMA((ring - 1, CROSS))],
        compiler_params=pltpu.CompilerParams(vmem_limit_bytes=VMEM_LIMIT),
        name="turned",
    )(*[pltpu.with_memory_space_constraint(part, pltpu.VMEM) for part in parts])


def row_total(parts):
    total = jnp.zeros(parts[0]().shape, jnp.float32)
    for part in parts:
        part = part().astype(jnp.float32)
        total = total + part * part
    return total


def inverse_scale(total):
    return jnp.broadcast_to(1.0 / jnp.sqrt(jnp.sum(total, axis=1, keepdims=True)), total.shape)


def first_kernel(parts_ref, out_ref, total_ref, out_vmem, sems):
    shards, experts, rows, lanes = parts_ref.shape
    blocks = rows // NORM_ROWS

    def copy(expert, block):
        at = (expert, pl.ds(block * NORM_ROWS, NORM_ROWS))
        return pltpu.make_async_copy(out_vmem.at[at], out_ref.at[at], sems.at[expert * blocks + block])

    for expert in range(experts):
        for block in range(blocks):
            at = pl.ds(block * NORM_ROWS, NORM_ROWS)
            total = row_total([lambda s=s: parts_ref[s, expert, at] for s in range(shards)])
            total_ref[expert, at] = total
            inverse = inverse_scale(total)
            for s in range(shards):
                part = parts_ref[s, expert, at].astype(jnp.float32)
                out_vmem[expert, at, pl.ds(s * lanes, lanes)] = (part * inverse).astype(jnp.bfloat16)
            copy(expert, block).start()
    for expert in range(experts):
        for block in range(blocks):
            copy(expert, block).wait()


def first_normed(parts, full_rows):
    shards, experts, rows, lanes = parts.shape
    width = shards * lanes
    return pl.pallas_call(
        first_kernel,
        in_specs=[pl.BlockSpec(memory_space=pltpu.VMEM)],
        out_specs=[pl.BlockSpec(memory_space=pltpu.HBM), pl.BlockSpec(memory_space=pltpu.VMEM)],
        out_shape=[
            pltpu.HBM((experts, full_rows, width), jnp.bfloat16),
            pltpu.VMEM((experts, rows, lanes), jnp.float32),
        ],
        scratch_shapes=[
            pltpu.VMEM((experts, rows, width), jnp.bfloat16),
            pltpu.SemaphoreType.DMA((experts * rows // NORM_ROWS,)),
        ],
        compiler_params=pltpu.CompilerParams(vmem_limit_bytes=VMEM_LIMIT),
        name="first",
    )(pltpu.with_memory_space_constraint(parts, pltpu.VMEM))


def column_at(j, i, lanes):
    me = lax.axis_index("shard")
    z, c = me >> 2, me & (CROSS - 1)
    place = (((z - j) & (RING - 1)) << 2) | ((c - i) & (CROSS - 1))
    return pl.ds(pl.multiple_of(place * lanes, lanes), lanes)


def router_kernel(*refs):
    tiles, (out_ref, router_vmem, sems) = refs[:RING], refs[RING:]
    columns = router_vmem.shape[0]
    lanes = tiles[0].shape[1]
    for j in range(RING):
        tile = tiles[j][...]
        for i in range(CROSS):
            router_vmem[:, column_at(j, i, lanes)] = tile[i * columns:(i + 1) * columns]
    copies = [pltpu.make_async_copy(router_vmem, out_ref.at[i], sems.at[i]) for i in range(out_ref.shape[0])]
    for copy in copies:
        copy.start()
    for copy in copies:
        copy.wait()


def router_copies(tiles, count):
    columns, lanes = tiles[0].shape[0] // CROSS, tiles[0].shape[1]
    width = RING * CROSS * lanes
    return pl.pallas_call(
        router_kernel,
        in_specs=[pl.BlockSpec(memory_space=pltpu.VMEM)] * RING,
        out_specs=pl.BlockSpec(memory_space=pltpu.HBM),
        out_shape=pltpu.HBM((count, columns, width), jnp.bfloat16),
        scratch_shapes=[
            pltpu.VMEM((columns, width), jnp.bfloat16),
            pltpu.SemaphoreType.DMA((count,)),
        ],
        compiler_params=pltpu.CompilerParams(vmem_limit_bytes=VMEM_LIMIT),
        name="router",
    )(*[pltpu.with_memory_space_constraint(tile, pltpu.VMEM) for tile in tiles])


def middle_kernel(*refs):
    parts, total_ref = refs[:-1], refs[-1]
    experts, rows, _ = total_ref.shape
    for expert in range(experts):
        for start, size in ((0, LAST_CUT), (LAST_CUT, rows - LAST_CUT)):
            at = pl.ds(expert * rows + start, size)
            total_ref[expert, pl.ds(start, size)] = row_total([lambda p=p, i=i: p[i, at] for p in parts for i in range(CROSS)])


def middle_totals(parts, experts):
    rows, lanes = parts[0].shape[1] // experts, parts[0].shape[2]
    return pl.pallas_call(
        middle_kernel,
        in_specs=[pl.BlockSpec(memory_space=pltpu.VMEM)] * len(parts),
        out_specs=pl.BlockSpec(memory_space=pltpu.VMEM),
        out_shape=pltpu.VMEM((experts, rows, lanes), jnp.float32),
        compiler_params=pltpu.CompilerParams(vmem_limit_bytes=VMEM_LIMIT),
        name="middle",
    )(*[pltpu.with_memory_space_constraint(part, pltpu.VMEM) for part in parts])


def last_kernel(first_ref, middle_ref, *refs):
    parts = refs[:RING]
    out_ref, scale_ref, out_vmem, total_vmem, scale_vmem, sems, scale_sem = refs[RING + 1:]
    experts, rows, _ = out_vmem.shape
    first, lanes = first_ref.shape[1:]
    cuts = ((0, LAST_CUT), (LAST_CUT, rows - LAST_CUT))

    def column(j, i):
        return column_at(j, i, lanes)

    def copy(expert, k):
        start, size = cuts[k]
        return pltpu.make_async_copy(
            out_vmem.at[expert, pl.ds(start, size)], out_ref.at[expert, pl.ds(first + start, size)], sems.at[expert, k]
        )

    scale_copy = pltpu.make_async_copy(scale_vmem, scale_ref, scale_sem)
    for expert in range(experts):
        total_vmem[expert, pl.ds(0, first)] = first_ref[expert]
        for k, (start, size) in enumerate(cuts):
            at = pl.ds(expert * rows + start, size)
            total = middle_ref[expert, pl.ds(start, size)] + row_total(
                [lambda j=j, i=i: parts[j][i, at] for j in LATE for i in range(CROSS)]
            )
            total_vmem[expert, pl.ds(first + start, size)] = total
            inverse = inverse_scale(total)
            for j in range(RING):
                for i in range(CROSS):
                    part = parts[j][i, at].astype(jnp.float32)
                    out_vmem[expert, pl.ds(start, size), column(j, i)] = (part * inverse).astype(jnp.bfloat16)
            copy(expert, k).start()
    for expert in range(experts):
        scale_vmem[pl.ds(expert, 1)] = jnp.sqrt(jnp.sum(jnp.transpose(total_vmem[expert]), axis=0, keepdims=True))
    scale_copy.start()
    for expert in range(experts):
        for k in range(len(cuts)):
            copy(expert, k).wait()
    scale_copy.wait()


def last_normed(totals, middle, parts, final):
    experts, full_rows, width = final.shape
    rows, lanes = full_rows - totals.shape[1], totals.shape[2]
    return pl.pallas_call(
        last_kernel,
        in_specs=[pl.BlockSpec(memory_space=pltpu.VMEM)] * (2 + RING)
        + [pl.BlockSpec(memory_space=pltpu.HBM)],
        out_specs=[pl.BlockSpec(memory_space=pltpu.HBM)] * 2,
        out_shape=[
            pltpu.HBM(final.shape, jnp.bfloat16),
            pltpu.HBM((experts, full_rows), jnp.float32),
        ],
        scratch_shapes=[
            pltpu.VMEM((experts, rows, width), jnp.bfloat16),
            pltpu.VMEM((experts, full_rows, lanes), jnp.float32),
            pltpu.VMEM((experts, full_rows), jnp.float32),
            pltpu.SemaphoreType.DMA((experts, 2)),
            pltpu.SemaphoreType.DMA,
        ],
        input_output_aliases={2 + RING: 0},
        compiler_params=pltpu.CompilerParams(vmem_limit_bytes=VMEM_LIMIT),
        name="last",
    )(*[pltpu.with_memory_space_constraint(x, pltpu.VMEM) for x in (totals, middle, *parts)], final)


def moved(x, dz, dx):
    pairs = [
        (z * CROSS + c, ((z + dz) % RING) * CROSS + (c + dx) % CROSS) for z in range(RING) for c in range(CROSS)
    ]
    return lax.ppermute(x, "shard", pairs)


def body(master_down, second_down, router_weight, router_gain):
    shards = lax.axis_size("shard")
    experts, rows, lanes = master_down.shape
    rows = rows // shards
    cut = (experts, shards, rows, lanes)
    master = pltpu.with_memory_space_constraint(master_down.reshape(cut), pltpu.HBM)
    second = pltpu.with_memory_space_constraint(second_down.reshape(cut), pltpu.HBM)
    me = lax.axis_index("shard")
    z, c = me >> 2, me & (CROSS - 1)
    steps = jnp.arange(shards, dtype=jnp.int32)
    targets = (((z + (steps & (RING - 1))) & (RING - 1)) << 2) | ((c + (steps >> 3)) & (CROSS - 1))
    sent = packed(master, second, FIRST_ROWS)
    received = lax.all_to_all(sent, "shard", 0, 0, tiled=True)
    pieces = [(router_weight * router_gain[:, None]).astype(jnp.bfloat16).T]
    for step in range(1, CROSS):
        pieces.append(moved(pieces[0], 0, step))
    tile = jnp.concatenate(pieces, axis=0)
    tiles = [tile] * RING
    for step in ALONG:
        tiles[step] = moved(tile, step, 0)
    parts = list(sorted_by_cross(targets, master, second, rows - FIRST_ROWS))
    for step in range(1, CROSS):
        parts[step] = moved(parts[step], 0, step)
    blocks = list(turned(parts))
    for step in ALONG:
        blocks[step] = moved(blocks[step], step, 0)
    copies = router_copies(tiles, lax.axis_size("expert"))
    gathered = lax.all_to_all(copies, "expert", 0, 0, tiled=True)
    final_down, totals = first_normed(received, rows)
    serve_router = gathered.reshape(-1, shards * lanes)
    middle = middle_totals([blocks[j] for j in range(RING) if j not in LATE], experts)
    final_down, scale_down = last_normed(totals, middle, blocks, final_down)
    return (final_down, scale_down, serve_router.T)


def solution(mesh):
    placed = (
        P("expert", None, "shard"),
        P("expert", None, "shard"),
        P("shard", "expert"),
        P("shard"),
    )
    return jax.shard_map(
        body,
        mesh=mesh,
        in_specs=placed,
        out_specs=(P("expert", "shard", None), P("expert", "shard"), P()),
        check_vma=False,
    )
```

```python
import jax
import jax.numpy as jnp
from jax import lax
from jax.experimental import pallas as pl
from jax.experimental.pallas import tpu as pltpu
from jax.sharding import PartitionSpec as P


RING, CROSS = 8, 4
LAST_CUT = 40
LATE = (1, 7)
FIRST_ROWS = 128
PACK_GROUPS = (16, 8, 4, 4)
NORM_ROWS = 32
VMEM_LIMIT = 32 << 20
ALONG = (4, 3, 5, 2, 6, 1, 7)


def merged(master, second):
    return (master + second.astype(jnp.float32)).astype(jnp.bfloat16)


def packed_kernel(master_ref, second_ref, out_ref, master_vmem, second_vmem, out_vmem, master_sem, second_sem, out_sem):
    rows = out_ref.shape[2]
    steps = len(PACK_GROUPS)

    def at(step):
        return pl.ds(sum(PACK_GROUPS[:step]), PACK_GROUPS[step])

    def copies(step):
        taken = (slice(None), at(step), pl.ds(0, rows))
        return (
            pltpu.make_async_copy(master_ref.at[taken], master_vmem.at[:, at(step)], master_sem.at[step]),
            pltpu.make_async_copy(second_ref.at[taken], second_vmem.at[:, at(step)], second_sem.at[step]),
        )

    def copy_out(step):
        return pltpu.make_async_copy(out_vmem.at[at(step)], out_ref.at[at(step)], out_sem.at[step])

    for step in range(steps):
        for copy in copies(step):
            copy.start()
    for step in range(steps):
        for copy in copies(step):
            copy.wait()
        for s in range(sum(PACK_GROUPS[:step]), sum(PACK_GROUPS[:step + 1])):
            out_vmem[s] = merged(master_vmem[:, s], second_vmem[:, s])
        copy_out(step).start()
    for step in range(steps):
        copy_out(step).wait()


def packed(master, second, rows):
    experts, shards, _, lanes = master.shape
    steps = len(PACK_GROUPS)
    return pl.pallas_call(
        packed_kernel,
        in_specs=[pl.BlockSpec(memory_space=pltpu.HBM)] * 2,
        out_specs=pl.BlockSpec(memory_space=pltpu.HBM),
        out_shape=pltpu.HBM((shards, experts, rows, lanes), jnp.bfloat16),
        scratch_shapes=[
            pltpu.VMEM((experts, shards, rows, lanes), jnp.float32),
            pltpu.VMEM((experts, shards, rows, lanes), jnp.bfloat16),
            pltpu.VMEM((shards, experts, rows, lanes), jnp.bfloat16),
            pltpu.SemaphoreType.DMA((steps,)),
            pltpu.SemaphoreType.DMA((steps,)),
            pltpu.SemaphoreType.DMA((steps,)),
        ],
        compiler_params=pltpu.CompilerParams(vmem_limit_bytes=VMEM_LIMIT),
        name="packed",
    )(master, second)


def sorted_kernel(targets, master_ref, second_ref, *refs):
    outs = refs[:CROSS]
    master_vmem, second_vmem, out_vmem, master_sem, second_sem, out_sem = refs[CROSS:]
    experts, shards, rows, _ = master_vmem.shape
    first = master_ref.shape[2] - rows

    def copies(s):
        taken = (slice(None), targets[s], pl.ds(first, rows))
        return (
            pltpu.make_async_copy(master_ref.at[taken], master_vmem.at[:, s], master_sem.at[s]),
            pltpu.make_async_copy(second_ref.at[taken], second_vmem.at[:, s], second_sem.at[s]),
        )

    def copy_out(i):
        return pltpu.make_async_copy(out_vmem.at[i - 1], outs[i], out_sem.at[i - 1])

    for s in range(shards):
        for copy in copies(s):
            copy.start()
    for i in range(CROSS):
        for j in range(RING):
            for copy in copies(i * RING + j):
                copy.wait()
            for expert in range(experts):
                kept = outs[0] if i == 0 else out_vmem.at[i - 1]
                kept[j, pl.ds(expert * rows, rows)] = merged(
                    master_vmem[expert, i * RING + j], second_vmem[expert, i * RING + j]
                )
        if i:
            copy_out(i).start()
    for i in range(1, CROSS):
        copy_out(i).wait()


def sorted_by_cross(targets, master, second, rows):
    experts, shards, _, lanes = master.shape
    block = (RING, experts * rows, lanes)
    return pl.pallas_call(
        sorted_kernel,
        in_specs=[pl.BlockSpec(memory_space=pltpu.SMEM)] + [pl.BlockSpec(memory_space=pltpu.HBM)] * 2,
        out_specs=[pl.BlockSpec(memory_space=pltpu.VMEM)] + [pl.BlockSpec(memory_space=pltpu.HBM)] * (CROSS - 1),
        out_shape=[pltpu.VMEM(block, jnp.bfloat16)] + [pltpu.HBM(block, jnp.bfloat16)] * (CROSS - 1),
        scratch_shapes=[
            pltpu.VMEM((experts, shards, rows, lanes), jnp.float32),
            pltpu.VMEM((experts, shards, rows, lanes), jnp.bfloat16),
            pltpu.VMEM((CROSS - 1, *block), jnp.bfloat16),
            pltpu.SemaphoreType.DMA((shards,)),
            pltpu.SemaphoreType.DMA((shards,)),
            pltpu.SemaphoreType.DMA((CROSS - 1,)),
        ],
        compiler_params=pltpu.CompilerParams(vmem_limit_bytes=VMEM_LIMIT),
        name="sorted",
    )(targets, master, second)


def turned_kernel(*refs):
    parts, outs, sems = refs[:CROSS], refs[CROSS:-1], refs[-1]
    copies = [
        pltpu.make_async_copy(parts[i].at[1 + j], out.at[i], sems.at[j, i])
        for j, out in enumerate(outs[1:])
        for i in range(CROSS)
    ]
    for copy in copies:
        copy.start()
    for i in range(CROSS):
        outs[0][i] = parts[i][0]
    for copy in copies:
        copy.wait()


def turned(parts):
    ring, rows, lanes = parts[0].shape
    block = (CROSS, rows, lanes)
    return pl.pallas_call(
        turned_kernel,
        in_specs=[pl.BlockSpec(memory_space=pltpu.VMEM)] * CROSS,
        out_specs=[pl.BlockSpec(memory_space=pltpu.VMEM)] + [pl.BlockSpec(memory_space=pltpu.HBM)] * (ring - 1),
        out_shape=[pltpu.VMEM(block, jnp.bfloat16)] + [pltpu.HBM(block, jnp.bfloat16)] * (ring - 1),
        scratch_shapes=[pltpu.SemaphoreType.DMA((ring - 1, CROSS))],
        compiler_params=pltpu.CompilerParams(vmem_limit_bytes=VMEM_LIMIT),
        name="turned",
    )(*[pltpu.with_memory_space_constraint(part, pltpu.VMEM) for part in parts])


def row_total(parts):
    total = jnp.zeros(parts[0]().shape, jnp.float32)
    for part in parts:
        part = part().astype(jnp.float32)
        total = total + part * part
    return total


def inverse_scale(total):
    return jnp.broadcast_to(1.0 / jnp.sqrt(jnp.sum(total, axis=1, keepdims=True)), total.shape)


def first_kernel(parts_ref, out_ref, total_ref, out_vmem, sems):
    shards, experts, rows, lanes = parts_ref.shape
    blocks = rows // NORM_ROWS

    def copy(expert, block):
        at = (expert, pl.ds(block * NORM_ROWS, NORM_ROWS))
        return pltpu.make_async_copy(out_vmem.at[at], out_ref.at[at], sems.at[expert * blocks + block])

    for expert in range(experts):
        for block in range(blocks):
            at = pl.ds(block * NORM_ROWS, NORM_ROWS)
            total = row_total([lambda s=s: parts_ref[s, expert, at] for s in range(shards)])
            total_ref[expert, at] = total
            inverse = inverse_scale(total)
            for s in range(shards):
                part = parts_ref[s, expert, at].astype(jnp.float32)
                out_vmem[expert, at, pl.ds(s * lanes, lanes)] = (part * inverse).astype(jnp.bfloat16)
            copy(expert, block).start()
    for expert in range(experts):
        for block in range(blocks):
            copy(expert, block).wait()


def first_normed(parts, full_rows):
    shards, experts, rows, lanes = parts.shape
    width = shards * lanes
    return pl.pallas_call(
        first_kernel,
        in_specs=[pl.BlockSpec(memory_space=pltpu.VMEM)],
        out_specs=[pl.BlockSpec(memory_space=pltpu.HBM), pl.BlockSpec(memory_space=pltpu.VMEM)],
        out_shape=[
            pltpu.HBM((experts, full_rows, width), jnp.bfloat16),
            pltpu.VMEM((experts, rows, lanes), jnp.float32),
        ],
        scratch_shapes=[
            pltpu.VMEM((experts, rows, width), jnp.bfloat16),
            pltpu.SemaphoreType.DMA((experts * rows // NORM_ROWS,)),
        ],
        compiler_params=pltpu.CompilerParams(vmem_limit_bytes=VMEM_LIMIT),
        name="first",
    )(pltpu.with_memory_space_constraint(parts, pltpu.VMEM))


def column_at(j, i, lanes):
    me = lax.axis_index("shard")
    z, c = me >> 2, me & (CROSS - 1)
    place = (((z - j) & (RING - 1)) << 2) | ((c - i) & (CROSS - 1))
    return pl.ds(pl.multiple_of(place * lanes, lanes), lanes)


def router_kernel(*refs):
    tiles, (out_ref, router_vmem, sems) = refs[:RING], refs[RING:]
    columns = router_vmem.shape[0]
    lanes = tiles[0].shape[1]
    for j in range(RING):
        tile = tiles[j][...]
        for i in range(CROSS):
            router_vmem[:, column_at(j, i, lanes)] = tile[i * columns:(i + 1) * columns]
    copies = [pltpu.make_async_copy(router_vmem, out_ref.at[i], sems.at[i]) for i in range(out_ref.shape[0])]
    for copy in copies:
        copy.start()
    for copy in copies:
        copy.wait()


def router_copies(tiles, count):
    columns, lanes = tiles[0].shape[0] // CROSS, tiles[0].shape[1]
    width = RING * CROSS * lanes
    return pl.pallas_call(
        router_kernel,
        in_specs=[pl.BlockSpec(memory_space=pltpu.VMEM)] * RING,
        out_specs=pl.BlockSpec(memory_space=pltpu.HBM),
        out_shape=pltpu.HBM((count, columns, width), jnp.bfloat16),
        scratch_shapes=[
            pltpu.VMEM((columns, width), jnp.bfloat16),
            pltpu.SemaphoreType.DMA((count,)),
        ],
        compiler_params=pltpu.CompilerParams(vmem_limit_bytes=VMEM_LIMIT),
        name="router",
    )(*[pltpu.with_memory_space_constraint(tile, pltpu.VMEM) for tile in tiles])


def middle_kernel(*refs):
    parts, total_ref = refs[:-1], refs[-1]
    experts, rows, _ = total_ref.shape
    for expert in range(experts):
        for start, size in ((0, LAST_CUT), (LAST_CUT, rows - LAST_CUT)):
            at = pl.ds(expert * rows + start, size)
            total_ref[expert, pl.ds(start, size)] = row_total([lambda p=p, i=i: p[i, at] for p in parts for i in range(CROSS)])


def middle_totals(parts, experts):
    rows, lanes = parts[0].shape[1] // experts, parts[0].shape[2]
    return pl.pallas_call(
        middle_kernel,
        in_specs=[pl.BlockSpec(memory_space=pltpu.VMEM)] * len(parts),
        out_specs=pl.BlockSpec(memory_space=pltpu.VMEM),
        out_shape=pltpu.VMEM((experts, rows, lanes), jnp.float32),
        compiler_params=pltpu.CompilerParams(vmem_limit_bytes=VMEM_LIMIT),
        name="middle",
    )(*[pltpu.with_memory_space_constraint(part, pltpu.VMEM) for part in parts])


def last_kernel(first_ref, middle_ref, *refs):
    parts = refs[:RING]
    out_ref, scale_ref, out_vmem, total_vmem, scale_vmem, sems, scale_sem = refs[RING + 1:]
    experts, rows, _ = out_vmem.shape
    first, lanes = first_ref.shape[1:]
    cuts = ((0, LAST_CUT), (LAST_CUT, rows - LAST_CUT))

    def column(j, i):
        return column_at(j, i, lanes)

    def copy(expert, k):
        start, size = cuts[k]
        return pltpu.make_async_copy(
            out_vmem.at[expert, pl.ds(start, size)], out_ref.at[expert, pl.ds(first + start, size)], sems.at[expert, k]
        )

    scale_copy = pltpu.make_async_copy(scale_vmem, scale_ref, scale_sem)
    for expert in range(experts):
        total_vmem[expert, pl.ds(0, first)] = first_ref[expert]
        for k, (start, size) in enumerate(cuts):
            at = pl.ds(expert * rows + start, size)
            total = middle_ref[expert, pl.ds(start, size)] + row_total(
                [lambda j=j, i=i: parts[j][i, at] for j in LATE for i in range(CROSS)]
            )
            total_vmem[expert, pl.ds(first + start, size)] = total
            inverse = inverse_scale(total)
            for j in range(RING):
                for i in range(CROSS):
                    part = parts[j][i, at].astype(jnp.float32)
                    out_vmem[expert, pl.ds(start, size), column(j, i)] = (part * inverse).astype(jnp.bfloat16)
            copy(expert, k).start()
    for expert in range(experts):
        scale_vmem[pl.ds(expert, 1)] = jnp.sqrt(jnp.sum(jnp.transpose(total_vmem[expert]), axis=0, keepdims=True))
    scale_copy.start()
    for expert in range(experts):
        for k in range(len(cuts)):
            copy(expert, k).wait()
    scale_copy.wait()


def last_normed(totals, middle, parts, final):
    experts, full_rows, width = final.shape
    rows, lanes = full_rows - totals.shape[1], totals.shape[2]
    return pl.pallas_call(
        last_kernel,
        in_specs=[pl.BlockSpec(memory_space=pltpu.VMEM)] * (2 + RING)
        + [pl.BlockSpec(memory_space=pltpu.HBM)],
        out_specs=[pl.BlockSpec(memory_space=pltpu.HBM)] * 2,
        out_shape=[
            pltpu.HBM(final.shape, jnp.bfloat16),
            pltpu.HBM((experts, full_rows), jnp.float32),
        ],
        scratch_shapes=[
            pltpu.VMEM((experts, rows, width), jnp.bfloat16),
            pltpu.VMEM((experts, full_rows, lanes), jnp.float32),
            pltpu.VMEM((experts, full_rows), jnp.float32),
            pltpu.SemaphoreType.DMA((experts, 2)),
            pltpu.SemaphoreType.DMA,
        ],
        input_output_aliases={2 + RING: 0},
        compiler_params=pltpu.CompilerParams(vmem_limit_bytes=VMEM_LIMIT),
        name="last",
    )(*[pltpu.with_memory_space_constraint(x, pltpu.VMEM) for x in (totals, middle, *parts)], final)


def moved(x, dz, dx):
    pairs = [
        (z * CROSS + c, ((z + dz) % RING) * CROSS + (c + dx) % CROSS) for z in range(RING) for c in range(CROSS)
    ]
    return lax.ppermute(x, "shard", pairs)


def body(master_down, second_down, router_weight, router_gain):
    shards = lax.axis_size("shard")
    experts, rows, lanes = master_down.shape
    rows = rows // shards
    cut = (experts, shards, rows, lanes)
    master = pltpu.with_memory_space_constraint(master_down.reshape(cut), pltpu.HBM)
    second = pltpu.with_memory_space_constraint(second_down.reshape(cut), pltpu.HBM)
    me = lax.axis_index("shard")
    z, c = me >> 2, me & (CROSS - 1)
    steps = jnp.arange(shards, dtype=jnp.int32)
    targets = (((z + (steps & (RING - 1))) & (RING - 1)) << 2) | ((c + (steps >> 3)) & (CROSS - 1))
    sent = packed(master, second, FIRST_ROWS)
    received = lax.all_to_all(sent, "shard", 0, 0, tiled=True)
    pieces = [(router_weight * router_gain[:, None]).astype(jnp.bfloat16).T]
    for step in range(1, CROSS):
        pieces.append(moved(pieces[0], 0, step))
    tile = jnp.concatenate(pieces, axis=0)
    tiles = [tile] * RING
    for step in ALONG:
        tiles[step] = moved(tile, step, 0)
    parts = list(sorted_by_cross(targets, master, second, rows - FIRST_ROWS))
    for step in range(1, CROSS):
        parts[step] = moved(parts[step], 0, step)
    blocks = list(turned(parts))
    for step in ALONG:
        blocks[step] = moved(blocks[step], step, 0)
    copies = router_copies(tiles, lax.axis_size("expert"))
    gathered = lax.all_to_all(copies, "expert", 0, 0, tiled=True)
    final_down, totals = first_normed(received, rows)
    serve_router = gathered.reshape(-1, shards * lanes)
    middle = middle_totals([blocks[j] for j in range(RING) if j not in LATE], experts)
    final_down, scale_down = last_normed(totals, middle, blocks, final_down)
    return (final_down, scale_down, serve_router.T)


def solution(mesh):
    placed = (
        P("expert", None, "shard"),
        P("expert", None, "shard"),
        P("shard", "expert"),
        P("shard"),
    )
    return jax.shard_map(
        body,
        mesh=mesh,
        in_specs=placed,
        out_specs=(P("expert", "shard", None), P("expert", "shard"), P()),
        check_vma=False,
    )
```
